32 devices in a mesh: ha: 8 (over z, core), wa: 2 (over y), ba: 2 (over x).
Axes of the slice: x: 2, y: 2, z: 4, core: 2. Of those that a mesh axis runs over, the one named last changes fastest.
Arguments:
- tokens: bfloat16 [2, 128, 64, 384], P('ba', 'ha', 'wa'), may hold values from -6 to 6
- cotangent: bfloat16 [2, 128, 64, 384], P('ba', 'ha', 'wa'), may hold values from -6 to 6
- w_qkv: bfloat16 [384, 1152], replicated, may hold values from -0.20412415 to 0.20412415
- w_proj: bfloat16 [384, 384], replicated, may hold values from -0.3125 to 0.3125
- table_logits: float32 [12, 225], replicated, may hold values from -6 to 6
- logit_scale: float32 [12], replicated, may hold values from 1 to 5.5
- gain: float32 [384], replicated, may hold values from 0.5 to 1.5
Outputs:
- d_tokens: bfloat16 [2, 128, 64, 384], P('ba', 'ha', 'wa')
- d_wqkv: float32 [384, 1152], P(None, 'ba')
- d_wproj: float32 [384, 384], P(None, 'ba')
- d_table: float32 [12, 225], replicated
- d_scale: float32 [12], replicated
- d_gain: float32 [384], replicated
The draws below stay inside these ranges and needn't reach their ends.
All inputs are finite; a program needn't handle non-finite values.
Results may differ from the reference program's by a relative error of at most 0.01.
The reference program's roundings to bfloat16 on the way count: a program that leaves them out, or rounds other values in their place, can miss the bound.
Values may be sent and summed in bfloat16 or wider, within the bound.
No kernel may reach another device: no remote copies, remote signals or barrier semaphores. Data moves between devices by JAX's collectives and lax.ppermute only.
A program may use at most 64 MiB of HBM per device.

```python
import math
import jax
import jax.numpy as jnp
from jax import lax

HEADS = 12
C = 384
WIN = 8
TABLE = 225
HEIGHT = 128
WIDTH = 64
BATCH = 2


def draw_w_qkv(key, part):
    spread = C ** (-0.5)
    base = jax.random.normal(key, (C, 3 * C), jnp.float32) * spread
    base = jnp.clip(base, -4.0 * spread, 4.0 * spread)
    return base.astype(jnp.bfloat16)


def shard_levels(key, shape, cuts, low, largest):
    factor_of, own = 1.0, jax.random.fold_in(key, 6)
    for dim, shards_of in cuts:
        heights = jnp.exp(jax.random.uniform(jax.random.fold_in(own, dim), (shards_of,), jnp.float32, low / len(cuts), largest / len(cuts)))
        factor_of = factor_of * jnp.repeat(heights, shape[dim] // shards_of).reshape([-1 if axis == dim else 1 for axis in range(len(shape))])
    return factor_of


def normal_values(own_key, shape, deviation, most, shards=(), kind=jnp.bfloat16):
    values = jax.random.normal(own_key, shape, jnp.float32) * deviation
    if len(shards) > 0:
        values = shard_levels(own_key, shape, shards, -0.22, 0.18) * values
    return jnp.clip(values, min=-most, max=most).astype(kind)


def setup_inputs(seed: int = 0) -> dict:
    splits = jax.random.split(jax.random.key(seed), 8)
    return {
        "tokens": normal_values(splits[0], (BATCH, HEIGHT, WIDTH, C), 1.0, 6.0, ((0, 2), (1, 8), (2, 2))),
        "cotangent": normal_values(splits[1], (BATCH, HEIGHT, WIDTH, C), 1.0, 6.0, ((0, 2), (1, 8), (2, 2))),
        "w_qkv": draw_w_qkv(jax.random.fold_in(splits[7], 71), 0),
        "w_proj": normal_values(splits[3], (C, C), C ** -0.5, 0.3125),
        "table_logits": normal_values(splits[4], (HEADS, TABLE), 1.5, 6.0, (), jnp.float32),
        "logit_scale": jnp.clip(jax.random.uniform(splits[5], (HEADS,), jnp.float32, 1.0, 5.5), 1.0, 5.5),
        "gain": jnp.clip(1.0 + 0.1 * jax.random.normal(splits[6], (C,), jnp.float32), 0.5, 1.5),
    }


EPS_NORM = 1e-05
MASK_FILL = -100.0
SCALE_CAP = math.log(100.0)
BIAS_RANGE = 16.0
HIGHEST = lax.Precision.HIGHEST

def coarse_product(form, left, right):
    return jnp.einsum(form, left.astype(jnp.float32), right.astype(jnp.float32), precision=HIGHEST)

def fine_product(form, left, right):
    return jnp.einsum(form, left, right, precision=HIGHEST)

def to_windows(block, window):
    images, height, width, depth = block.shape
    tiles = block.reshape(images, height // window, window, width // window, window, depth)
    tiles = tiles.transpose(0, 1, 3, 2, 4, 5)
    return tiles.reshape(images, height // window * (width // window), window * window, depth)

def from_windows(tiles, images, height, width, window):
    depth = tiles.shape[-1]
    grid = tiles.reshape(images, height // window, width // window, window, window, depth)
    return grid.transpose(0, 1, 3, 2, 4, 5).reshape(images, height, width, depth)

def position_onehot(window):
    places = jnp.arange(window * window, dtype=jnp.int32)
    row_of = places // window
    col_of = places % window
    offset = (row_of[:, None] - row_of[None, :] + window - 1) * (2 * window - 1) + (col_of[:, None] - col_of[None, :] + window - 1)
    entries = jnp.arange((2 * window - 1) ** 2, dtype=jnp.int32)
    return (offset.reshape(-1)[:, None] == entries[None, :]).astype(jnp.float32)

def region_of(coords, extent, window):
    return (coords >= extent - window).astype(jnp.int32) + (coords >= extent - window // 2).astype(jnp.int32)

def region_mask(row_start, col_start, rows, cols, height, width, window):
    row_label = region_of(row_start + jnp.arange(rows, dtype=jnp.int32), height, window)
    col_label = region_of(col_start + jnp.arange(cols, dtype=jnp.int32), width, window)
    labels = row_label[:, None] * 3 + col_label[None, :]
    labels = labels.reshape(rows // window, window, cols // window, window).transpose(0, 2, 1, 3)
    labels = labels.reshape(-1, window * window)
    return jnp.where(labels[:, :, None] != labels[:, None, :], MASK_FILL, 0.0).astype(jnp.float32)

def grads_region(block, grad_block, row_start, col_start, height, width, window, params):
    w_qkv, w_proj, table_logits, logit_scale, gain = params
    images, rows, cols, depth = block.shape
    heads = logit_scale.shape[0]
    head_dim = depth // heads
    tiles = to_windows(block, window)
    grad_tiles = to_windows(grad_block, window)
    count = tiles.shape[1]
    length = window * window
    flat = tiles.reshape(-1, depth)
    qkv = jnp.dot(flat, w_qkv, preferred_element_type=jnp.float32).astype(jnp.bfloat16)
    qkv = qkv.reshape(images, count, length, 3, heads, head_dim)
    query = qkv[:, :, :, 0].astype(jnp.float32)
    keys = qkv[:, :, :, 1].astype(jnp.float32)
    values = qkv[:, :, :, 2]
    query_inv = lax.rsqrt(lax.optimization_barrier(jnp.sum(query * query, -1, keepdims=True)) + 1.0)
    key_inv = lax.rsqrt(lax.optimization_barrier(jnp.sum(keys * keys, -1, keepdims=True)) + 1.0)
    unit_query = query * query_inv
    unit_key = keys * key_inv
    scale = jnp.exp(jnp.minimum(logit_scale, SCALE_CAP))
    onehot = position_onehot(window)
    sigma = jax.nn.sigmoid(table_logits)
    rel_bias = jnp.dot(sigma * BIAS_RANGE, onehot.T, precision=HIGHEST).reshape(heads, length, length)
    mask = region_mask(row_start, col_start, rows, cols, height, width, window)
    cosine = fine_product('bnqhd,bnkhd->bnhqk', unit_query, unit_key)
    scores = scale[:, None, None] * cosine + rel_bias[None, None] + mask[None, :, None]
    top = lax.optimization_barrier(jnp.max(scores, -1, keepdims=True))
    expo = jnp.exp(scores - top)
    probs = expo / lax.optimization_barrier(jnp.sum(expo, -1, keepdims=True))
    probs_low = probs.astype(jnp.bfloat16)
    attended = coarse_product('bnhqk,bnkhd->bnqhd', probs_low, values).astype(jnp.bfloat16).reshape(-1, depth)
    proj = jnp.dot(attended, w_proj, preferred_element_type=jnp.float32)
    centre = proj - lax.optimization_barrier(jnp.mean(proj, -1, keepdims=True))
    inv_std = lax.rsqrt(lax.optimization_barrier(jnp.mean(centre * centre, -1, keepdims=True)) + EPS_NORM)
    normed = centre * inv_std
    upstream = grad_tiles.reshape(-1, depth).astype(jnp.float32)
    d_gain = lax.optimization_barrier(jnp.sum(upstream * normed, 0))
    scaled = upstream * gain
    d_proj = inv_std * (scaled - lax.optimization_barrier(jnp.mean(scaled, -1, keepdims=True)) - normed * lax.optimization_barrier(jnp.mean(scaled * normed, -1, keepdims=True)))
    d_proj = d_proj.astype(jnp.bfloat16)
    d_wproj = jnp.dot(attended.T, d_proj, preferred_element_type=jnp.float32)
    d_att = jnp.dot(d_proj, w_proj.T, preferred_element_type=jnp.float32).astype(jnp.bfloat16)
    d_att = d_att.reshape(images, count, length, heads, head_dim)
    d_probs = coarse_product('bnqhd,bnkhd->bnhqk', d_att, values)
    d_values = coarse_product('bnhqk,bnqhd->bnkhd', probs_low, d_att)
    d_scores = probs * (d_probs - lax.optimization_barrier(jnp.sum(d_probs * probs, -1, keepdims=True)))
    d_bias = lax.optimization_barrier(jnp.sum(d_scores, (0, 1))).reshape(heads, length * length)
    d_table = jnp.dot(d_bias, onehot, precision=HIGHEST) * (BIAS_RANGE * sigma * (1.0 - sigma))
    live = (logit_scale < SCALE_CAP).astype(jnp.float32)
    d_scale = lax.optimization_barrier(jnp.sum(d_scores * cosine, (0, 1, 3, 4))) * scale * live
    d_cos = d_scores * scale[:, None, None]
    d_unit_q = fine_product('bnhqk,bnkhd->bnqhd', d_cos, unit_key)
    d_unit_k = fine_product('bnhqk,bnqhd->bnkhd', d_cos, unit_query)
    d_query = query_inv * (d_unit_q - unit_query * lax.optimization_barrier(jnp.sum(unit_query * d_unit_q, -1, keepdims=True)))
    d_key = key_inv * (d_unit_k - unit_key * lax.optimization_barrier(jnp.sum(unit_key * d_unit_k, -1, keepdims=True)))
    d_qkv = jnp.stack([d_query, d_key, d_values], 3).astype(jnp.bfloat16).reshape(-1, 3 * depth)
    d_wqkv = jnp.dot(flat.T, d_qkv, preferred_element_type=jnp.float32)
    d_flat = jnp.dot(d_qkv, w_qkv.T, preferred_element_type=jnp.float32).astype(jnp.bfloat16)
    d_block = from_windows(d_flat.reshape(images, count, length, depth), images, rows, cols, window)
    return (d_block, (d_wqkv, d_wproj, d_table, d_scale, d_gain))

def reference(tokens, cotangent, w_qkv, w_proj, table_logits, logit_scale, gain):
    shift = WIN // 2
    images, height, width, depth = tokens.shape
    moved = jnp.roll(tokens, (-shift, -shift), axis=(1, 2))
    moved_grad = jnp.roll(cotangent, (-shift, -shift), axis=(1, 2))
    params = (w_qkv, w_proj, table_logits, logit_scale, gain)
    bands = height // WIN
    anchor = jnp.zeros((), jnp.int32)

    def one_band(totals, index):
        image = (index // bands).astype(jnp.int32)
        start = (index % bands * WIN).astype(jnp.int32)
        block = lax.dynamic_slice(moved, (image, start, anchor, anchor), (1, WIN, width, depth))
        grad_block = lax.dynamic_slice(moved_grad, (image, start, anchor, anchor), (1, WIN, width, depth))
        d_block, parts = grads_region(block, grad_block, start, anchor, height, width, WIN, params)
        return (jax.tree.map(jnp.add, totals, parts), d_block[0])
    initial = (jnp.zeros((depth, 3 * depth), jnp.float32), jnp.zeros((depth, depth), jnp.float32), jnp.zeros(table_logits.shape, jnp.float32), jnp.zeros(logit_scale.shape, jnp.float32), jnp.zeros(gain.shape, jnp.float32))
    totals, pieces = lax.scan(one_band, initial, jnp.arange(images * bands, dtype=jnp.int32))
    d_moved = pieces.reshape(images, height, width, depth)
    back = jnp.roll(d_moved, (shift, shift), axis=(1, 2))
    d_tokens = (cotangent.astype(jnp.float32) + back.astype(jnp.float32)).astype(jnp.bfloat16)
    return (d_tokens, totals[0], totals[1], totals[2], totals[3], totals[4])
```

```python
import math

import jax
import jax.numpy as jnp
from jax import lax
from jax.experimental import pallas as pl
from jax.experimental.pallas import tpu as pltpu
from jax.sharding import Mesh
from jax.sharding import PartitionSpec as P

WIN = 8
TOKENS = WIN * WIN
LANES = 128
EPS_NORM = 1e-05
MASK_FILL = -100.0
SCALE_CAP = math.log(100.0)
BIAS_RANGE = 16.0
F32 = jnp.float32
BF16 = jnp.bfloat16


def dot_nn(left, right):
    return lax.dot_general(left, right, (((1,), (0,)), ((), ())), preferred_element_type=F32)


def dot_nt(left, right):
    return lax.dot_general(left, right, (((1,), (1,)), ((), ())), preferred_element_type=F32)


def dot_tn(left, right):
    return lax.dot_general(left, right, (((0,), (0,)), ((), ())), preferred_element_type=F32)


def iota(shape, dim):
    return lax.broadcasted_iota(jnp.int32, shape, dim)


def split(value):
    high = value.astype(BF16)
    return high, (value - high.astype(F32)).astype(BF16)


def group_sum(value, ones):
    high, low = split(value)
    width = ones.shape[0]
    parts = []
    for start in range(0, value.shape[1], width):
        part = slice(start, start + width)
        parts.append(dot_nn(high[:, part], ones) + dot_nn(low[:, part], ones))
    return jnp.concatenate(parts, axis=1)


def make_kernel(rows, cols, depth, heads):
    head_dim = depth // heads
    per_tile = LANES // head_dim
    groups = heads // per_tile
    col_windows = cols // WIN
    row_windows = rows // WIN
    pairs = row_windows * col_windows // 2
    pairs_across = col_windows // 2
    stacked = per_tile * TOKENS
    small_at = 6 * depth

    def kernel(
        flags,
        img,
        w_qkv,
        w_proj,
        table_a,
        table_b,
        gain,
        scale,
        d_img,
        grads,
        xf,
        uf,
        xb,
        qk_raw,
        inv,
        q_hi,
        q_lo,
        k_hi,
        k_lo,
        val,
        prob,
        raw,
        att,
        d_prj,
        d_att,
        d_qkv,
        d_unit,
        bias,
        d_bias,
        d_sc,
        d_gn,
        small,
    ):
        half = iota((1, LANES), 1) < TOKENS
        for i in range(rows):
            for j in range(col_windows):
                at = (i // WIN * col_windows + j) * TOKENS + i % WIN * WIN
                xf[at : at + WIN, :] = img[0, i, j * WIN : (j + 1) * WIN, :].astype(F32)
                uf[at : at + WIN, :] = img[1, i, j * WIN : (j + 1) * WIN, :].astype(F32)
        sub = iota((WIN, LANES), 0)
        lane = iota((WIN, LANES), 1)
        for h in range(heads):
            near = jnp.broadcast_to(table_a[h : h + 1, :], (WIN, LANES))
            far = jnp.broadcast_to(table_b[h : h + 1, :], (WIN, LANES))
            near = pltpu.roll(near, LANES - WIN + 1, 1, stride=1, stride_axis=0)
            far = pltpu.roll(far, 1, 1, stride=1, stride_axis=0)
            line = jnp.where(lane % WIN <= sub, near, far)
            for r in range(WIN):
                first = pltpu.roll(line, (LANES - (WIN - 1 - r) * WIN) % LANES, 1)
                second = pltpu.roll(line, (LANES + TOKENS - (WIN - 1 - r) * WIN) % LANES, 1)
                at = h * TOKENS + r * WIN
                bias[at : at + WIN, :] = jnp.where(half, first, second)
        d_bias[...] = jnp.zeros_like(d_bias)
        d_sc[...] = jnp.zeros_like(d_sc)
        d_gn[...] = jnp.zeros_like(d_gn)

        wide = 2 * LANES
        ones = (iota((wide, wide), 0) // head_dim == iota((wide, wide), 1) // head_dim).astype(F32)
        ones = ones.astype(BF16)
        owner = iota((1, wide), 1) % LANES // head_dim
        head_f32 = [(owner == h).astype(F32) for h in range(per_tile)]
        head_low = [m.astype(BF16) for m in head_f32]
        top_rows = (iota((2 * TOKENS, LANES), 0) < TOKENS).astype(F32)
        top_rows, low_rows = top_rows.astype(BF16), (1.0 - top_rows).astype(BF16)

        key = iota((TOKENS, LANES), 0)
        query = iota((TOKENS, LANES), 1) % TOKENS
        edge = WIN // 2
        split_r = ((key // WIN) >= edge) != ((query // WIN) >= edge)
        split_c = ((key % WIN) >= edge) != ((query % WIN) >= edge)
        split_c = jnp.logical_and(split_c, iota((TOKENS, LANES), 1) >= TOKENS)
        mask_r = jnp.where(split_r, MASK_FILL, 0.0)
        mask_c = jnp.where(split_c, MASK_FILL, 0.0)

        def beside(ref, at, tile):
            one = ref[pl.ds(at, TOKENS), tile]
            two = ref[pl.ds(at + TOKENS, TOKENS), tile]
            return jnp.concatenate([one, two], axis=1)

        def stack(block):
            return jnp.concatenate([block * head_low[h] for h in range(per_tile)], axis=0)

        def diagonal(ref, at, tile):
            block = ref[pl.ds(at, 2 * TOKENS), tile]
            return jnp.concatenate([block * top_rows, block * low_rows], axis=1)

        def gather_heads(out):
            total = out[:TOKENS] * head_f32[0]
            for h in range(1, per_tile):
                total = total + out[h * TOKENS : (h + 1) * TOKENS] * head_f32[h]
            return total

        def forward(p, carry):
            at = pl.multiple_of(p * 2 * TOKENS, 2 * TOKENS)
            span = pl.ds(at, 2 * TOKENS)
            x = xf[span, :].astype(BF16)
            xb[span, :] = x
            qkv = dot_nn(x, w_qkv[...]).astype(BF16)
            val[span, :] = qkv[:, 2 * depth :]
            both = qkv[:, : 2 * depth].astype(F32)
            root = lax.rsqrt(group_sum(both * both, ones) + 1.0)
            unit = both * root
            qk_raw[span, :] = unit
            inv[span, :] = root
            high, low = split(unit[:, :depth] * scale[...])
            q_hi[span, :] = high
            q_lo[span, :] = low
            high, low = split(unit[:, depth:])
            k_hi[span, :] = high
            k_lo[span, :] = low
            row_edge = jnp.where(p // pairs_across == row_windows - 1, flags[0], 0)
            col_edge = jnp.where(p % pairs_across == pairs_across - 1, flags[1], 0)
            mask = jnp.minimum(mask_r * row_edge.astype(F32), mask_c * col_edge.astype(F32))
            for g in range(groups):
                tile = slice(g * LANES, (g + 1) * LANES)
                keys = stack(beside(k_hi, at, tile))
                keys_low = stack(beside(k_lo, at, tile))
                queries = diagonal(q_hi, at, tile)
                score = dot_nt(keys, queries) + (
                    dot_nt(keys_low, queries) + dot_nt(keys, diagonal(q_lo, at, tile))
                )
                raw[p, g] = score
                lows = []
                for h in range(per_tile):
                    place = slice(h * TOKENS, (h + 1) * TOKENS)
                    of = (g * per_tile + h) * TOKENS
                    s = score[place] + bias[of : of + TOKENS, :] + mask
                    e = jnp.exp(s - jnp.max(s, axis=0, keepdims=True))
                    pr = e * (1.0 / jnp.sum(e, axis=0, keepdims=True))
                    prob[p, g, place, :] = pr
                    lows.append(pr.astype(BF16))
                out = dot_tn(jnp.concatenate(lows, axis=0), stack(beside(val, at, tile)))
                att[pl.ds(at, TOKENS), tile] = out[:TOKENS, :LANES].astype(BF16)
                att[pl.ds(at + TOKENS, TOKENS), tile] = out[TOKENS:, LANES:].astype(BF16)
            proj = dot_nn(att[span, :], w_proj[...])
            centre = proj - jnp.mean(proj, -1, keepdims=True)
            std = lax.rsqrt(jnp.mean(centre * centre, -1, keepdims=True) + EPS_NORM)
            normed = centre * std
            up = uf[span, :]
            prod = up * normed
            d_gn[...] += jnp.sum(prod, axis=0, keepdims=True)
            u = up * gain[...]
            d_p = std * (
                u - jnp.mean(u, -1, keepdims=True) - normed * jnp.mean(u * normed, -1, keepdims=True)
            )
            d_p = d_p.astype(BF16)
            d_prj[span, :] = d_p
            d_att[span, :] = dot_nt(d_p, w_proj[...]).astype(BF16)
            return carry

        lax.fori_loop(0, pairs, forward, 0)

        def backward(p, carry):
            at = pl.multiple_of(p * 2 * TOKENS, 2 * TOKENS)
            span = pl.ds(at, 2 * TOKENS)
            for g in range(groups):
                tile = slice(g * LANES, (g + 1) * LANES)
                key_tile = slice(depth + g * LANES, depth + (g + 1) * LANES)
                val_tile = slice(2 * depth + g * LANES, 2 * depth + (g + 1) * LANES)
                values = stack(beside(val, at, tile))
                ups = diagonal(d_att, at, tile)
                d_pr = dot_nt(values, ups)
                lows, d_lows = [], []
                for h in range(per_tile):
                    place = slice(h * TOKENS, (h + 1) * TOKENS)
                    of = (g * per_tile + h) * TOKENS
                    pr = prob[p, g, place, :]
                    pd = pr * d_pr[place]
                    d_s = pd - pr * jnp.sum(pd, axis=0, keepdims=True)
                    d_bias[of : of + TOKENS, :] += d_s
                    by_scale = jnp.sum(d_s * raw[p, g, place, :], axis=0, keepdims=True)
                    head = g * per_tile + h
                    d_sc[head : head + 1, :] += by_scale
                    lows.append(pr.astype(BF16))
                    d_lows.append(d_s.astype(BF16))
                low = jnp.concatenate(lows, axis=0)
                d_low = jnp.concatenate(d_lows, axis=0)
                d_v = gather_heads(dot_nn(low, ups)).astype(BF16)
                d_qkv[pl.ds(at, TOKENS), val_tile] = d_v[:, :LANES]
                d_qkv[pl.ds(at + TOKENS, TOKENS), val_tile] = d_v[:, LANES:]
                d_k = gather_heads(dot_nn(d_low, diagonal(q_hi, at, tile)))
                d_unit[:TOKENS, key_tile] = d_k[:, :LANES]
                d_unit[TOKENS:, key_tile] = d_k[:, LANES:]
                d_q = dot_tn(d_low, stack(beside(k_hi, at, tile)))
                d_unit[:TOKENS, tile] = d_q[:TOKENS, :LANES] * scale[:, tile]
                d_unit[TOKENS:, tile] = d_q[TOKENS:, LANES:] * scale[:, tile]
            unit = qk_raw[span, :]
            d_u = d_unit[...]
            d_qk = inv[span, :] * (d_u - unit * group_sum(unit * d_u, ones))
            d_qkv[span, : 2 * depth] = d_qk.astype(BF16)
            flat = dot_nt(d_qkv[span, :], w_qkv[...])
            row_at = p // pairs_across * WIN
            for w in range(2):
                col_at = pl.multiple_of((p % pairs_across * 2 + w) * WIN, WIN)
                for r in range(WIN):
                    piece = flat[w * TOKENS + r * WIN : w * TOKENS + (r + 1) * WIN]
                    d_img[row_at + r, pl.ds(col_at, WIN), :] = piece.astype(BF16)
            return carry

        lax.fori_loop(0, pairs, backward, 0)

        d_wp = dot_tn(att[...], d_prj[...])
        d_wq = dot_tn(xb[...], d_qkv[...])
        side = 9 * LANES // 2
        full = side // LANES
        turned = pltpu.roll(d_wp[:, LANES : 2 * LANES], TOKENS, 1)
        middle = d_wq[:, full * LANES : (full + 1) * LANES]
        for j in range(full):
            place = slice(j * depth, (j + 1) * depth)
            grads[0, place, :] = d_wq[:, j * LANES : (j + 1) * LANES].astype(BF16)
            other = full + 1 + j
            grads[1, place, :] = d_wq[:, other * LANES : (other + 1) * LANES].astype(BF16)
        place = slice(full * depth, (full + 1) * depth)
        grads[0, place, :] = jnp.where(half, middle, turned).astype(BF16)
        grads[1, place, :] = jnp.where(half, turned, middle).astype(BF16)
        place = slice((full + 1) * depth, (full + 2) * depth)
        grads[0, place, :] = d_wp[:, :LANES].astype(BF16)
        grads[1, place, :] = d_wp[:, 2 * LANES :].astype(BF16)

        small[...] = jnp.zeros_like(small)
        for h in range(heads):
            line = jnp.zeros((WIN, LANES), F32)
            for r in range(WIN):
                at = h * TOKENS + r * WIN
                part = d_bias[at : at + WIN, :]
                part = jnp.where(half, part + pltpu.roll(part, TOKENS, 1), 0.0)
                line = line + pltpu.roll(part, (WIN - 1 - r) * WIN, 1)
            near, far = jnp.zeros_like(line), jnp.zeros_like(line)
            for c in range(WIN):
                own = jnp.where(sub == c, line, 0.0)
                near = near + pltpu.roll(own, WIN - 1 - c, 1)
                far = far + pltpu.roll(own, LANES - 1 - c, 1)
            near = jnp.where(lane % WIN >= WIN - 1 - sub, near, 0.0)
            far = jnp.where(lane % WIN + sub + 1 <= WIN - 1, far, 0.0)
            small[h : h + 1, :] = jnp.sum(near, axis=0, keepdims=True)
            small[heads + h : heads + h + 1, :] = jnp.sum(far, axis=0, keepdims=True)
        for j in range(groups):
            small[2 * heads + j : 2 * heads + j + 1, :] = d_gn[:, j * LANES : (j + 1) * LANES]
        sums = jnp.zeros((1, LANES), F32)
        for h in range(heads):
            total = jnp.sum(d_sc[h : h + 1, :], axis=1, keepdims=True)
            sums = sums + jnp.where(iota((1, LANES), 1) == h, total, 0.0)
        at = 2 * heads + groups
        small[at : at + 1, :] = sums
        grads[0, small_at:, :] = small[...].astype(BF16)
        grads[1, small_at:, :] = small[...].astype(BF16)

    tokens = rows * cols

    def call(flags, img, w_qkv, w_proj, table_a, table_b, gain, scale, sent_rows):
        vmem = pltpu.VMEM
        scratch = [
            vmem((tokens, depth), F32),
            vmem((tokens, depth), F32),
            vmem((tokens, depth), BF16),
            vmem((tokens, 2 * depth), F32),
            vmem((tokens, 2 * depth), F32),
            vmem((tokens, depth), BF16),
            vmem((tokens, depth), BF16),
            vmem((tokens, depth), BF16),
            vmem((tokens, depth), BF16),
            vmem((tokens, depth), BF16),
            vmem((pairs, groups, stacked, LANES), F32),
            vmem((pairs, groups, stacked, LANES), F32),
            vmem((tokens, depth), BF16),
            vmem((tokens, depth), BF16),
            vmem((tokens, depth), BF16),
            vmem((tokens, 3 * depth), BF16),
            vmem((2 * TOKENS, 2 * depth), F32),
            vmem((heads * TOKENS, LANES), F32),
            vmem((heads * TOKENS, LANES), F32),
            vmem((16, LANES), F32),
            vmem((1, depth), F32),
            vmem((sent_rows - small_at, LANES), F32),
        ]
        return pl.pallas_call(
            kernel,
            out_shape=(
                jax.ShapeDtypeStruct((rows, cols, depth), BF16),
                jax.ShapeDtypeStruct((2, sent_rows, LANES), BF16),
            ),
            in_specs=[pl.BlockSpec(memory_space=pltpu.SMEM)]
            + [pl.BlockSpec(memory_space=pltpu.VMEM)] * 7,
            out_specs=(
                pl.BlockSpec(memory_space=pltpu.VMEM),
                pl.BlockSpec(memory_space=pltpu.VMEM),
            ),
            scratch_shapes=scratch,
            name="block_grads",
        )(flags, img, w_qkv, w_proj, table_a, table_b, gain, scale)

    return call


def route(axes, move):
    sizes = [lax.axis_size(a) for a in axes]
    pairs = []
    for flat in range(math.prod(sizes)):
        left, where = flat, []
        for size in reversed(sizes):
            where.append(left % size)
            left //= size
        where = move(where[::-1], sizes)
        target = 0
        for place, size in zip(where, sizes):
            target = target * size + place
        pairs.append((flat, target))
    return pairs


GRID = ("hz", "hc", "wa")


def step(rows, cols):
    def move(where, sizes):
        high = (where[0] * sizes[1] + where[1] + rows) % (sizes[0] * sizes[1])
        return [high // sizes[1], high % sizes[1], (where[2] + cols) % sizes[2]]

    return move


def shards(tokens, cotangent, w_qkv, w_proj, table_logits, logit_scale, gain):
    images, rows, cols, depth = tokens.shape
    heads = logit_scale.shape[0]
    span = 2 * WIN - 1
    edge = WIN // 2
    both = jnp.concatenate([tokens, cotangent], 0)
    below = lax.ppermute(both[:, :edge], GRID, route(GRID, step(-1, 0)))
    beside = lax.ppermute(both[:, :, :edge], GRID, route(GRID, step(0, -1)))
    corner = lax.ppermute(both[:, :edge, :edge], GRID, route(GRID, step(-1, -1)))
    main = jnp.concatenate([both[:, edge:, edge:], beside[:, edge:]], 2)
    last = jnp.concatenate([below[:, :, edge:], corner], 2)
    moved = jnp.concatenate([main, last], 1)

    ha = lax.axis_index("hz") * lax.axis_size("hc") + lax.axis_index("hc")
    flags = jnp.stack(
        [
            (ha == lax.axis_size("hz") * lax.axis_size("hc") - 1).astype(jnp.int32),
            (lax.axis_index("wa") == lax.axis_size("wa") - 1).astype(jnp.int32),
        ]
    )
    scale = jnp.exp(jnp.minimum(logit_scale, SCALE_CAP))
    scale = jnp.repeat(scale, depth // heads)[None]
    sigma = jax.nn.sigmoid(table_logits)
    table = (sigma * BIAS_RANGE).reshape(heads, span, span)
    table_a = table[:, :, :WIN].reshape(heads, span * WIN)
    table_b = jnp.pad(table[:, :, WIN:], ((0, 0), (0, 0), (0, 1))).reshape(heads, span * WIN)
    fill = ((0, 0), (0, LANES - span * WIN))
    table_a, table_b = jnp.pad(table_a, fill), jnp.pad(table_b, fill)

    cores, tall, across = lax.axis_size("hc"), lax.axis_size("hz"), lax.axis_size("wa")
    owners = cores * tall * across
    body = 6 * depth
    used = body + 2 * heads + depth // LANES + 1
    unit = 8 * owners
    sent = -(-used // unit) * unit
    call = make_kernel(rows, cols, depth, heads)
    d_moved, grads = call(
        flags, moved, w_qkv, w_proj, table_a, table_b, gain[None], scale, sent
    )

    right = lax.ppermute(d_moved[: rows - edge, cols - edge :], GRID, route(GRID, step(0, 1)))
    lower = lax.ppermute(d_moved[rows - edge :, : cols - edge], GRID, route(GRID, step(1, 0)))
    cross = lax.ppermute(
        d_moved[rows - edge :, cols - edge :], GRID, route(GRID, step(1, 1))
    )
    upper = jnp.concatenate([cross, lower], 1)
    main = jnp.concatenate([right, d_moved[: rows - edge, : cols - edge]], 1)
    back = jnp.concatenate([upper, main], 0)[None]
    d_tokens = (cotangent.astype(F32) + back.astype(F32)).astype(BF16)

    core = lax.axis_index("hc")
    grads = grads.reshape(2, cores, sent // cores, LANES)
    mine = lax.dynamic_index_in_dim(grads, core, 1, keepdims=False)
    given = lax.dynamic_index_in_dim(grads, 1 - core, 1, keepdims=False)
    swap = route(("hc",), lambda where, sizes: [1 - where[0]])
    taken = lax.ppermute(given, "hc", swap)
    summed = (mine.astype(F32) + taken.astype(F32)).astype(BF16)
    piece = sent // owners
    summed = summed.reshape(2 * tall * across, piece, LANES)
    parts = lax.all_to_all(summed, ("ba", "hz", "wa"), 0, 0, tiled=True)
    total = parts.astype(F32).sum(0).astype(BF16)
    spread = jnp.broadcast_to(total[None], (tall * across, piece, LANES))
    ours = lax.all_to_all(spread, ("hz", "wa"), 0, 0, tiled=True)
    ours = ours.reshape(sent // cores, LANES)
    theirs = lax.ppermute(ours, "hc", swap)
    first = jnp.where(core == 0, ours, theirs)
    second = jnp.where(core == 0, theirs, ours)
    whole = jnp.concatenate([first, second], 0).astype(F32)
    tiles = [whole[j * depth : (j + 1) * depth] for j in range(6)]
    mid = tiles[4]
    low, high = mid[:, :TOKENS], mid[:, TOKENS:]
    image = lax.axis_index("ba")
    d_wqkv = jnp.where(
        image == 0,
        jnp.concatenate(tiles[:4] + [low], 1),
        jnp.concatenate([high] + tiles[:4], 1),
    )
    d_wproj = jnp.where(
        image == 0,
        jnp.concatenate([tiles[5], high], 1),
        jnp.concatenate([low, tiles[5]], 1),
    )
    small = whole[body:]
    near = small[:heads, : span * WIN].reshape(heads, span, WIN)
    far = small[heads : 2 * heads, : span * WIN].reshape(heads, span, WIN)
    d_table = jnp.concatenate([near, far[:, :, : WIN - 1]], 2).reshape(heads, span * span)
    d_table = d_table * (BIAS_RANGE * sigma * (1.0 - sigma))
    d_gain = small[2 * heads : 2 * heads + depth // LANES].reshape(depth)
    d_scale = small[2 * heads + depth // LANES, :heads]
    d_scale = jnp.where(logit_scale < SCALE_CAP, d_scale, 0.0)
    return (d_tokens, d_wqkv, d_wproj, d_table, d_scale, d_gain)


def solution(mesh):
    sizes = mesh.shape
    devices = mesh.devices.reshape(sizes["ha"] // 2, 2, sizes["wa"], sizes["ba"])
    inner = Mesh(devices, ("hz", "hc", "wa", "ba"))
    image = P("ba", ("hz", "hc"), "wa", None)
    return jax.shard_map(
        shards,
        mesh=inner,
        in_specs=(image, image, P(), P(), P(), P(), P()),
        out_specs=(image, P(None, "ba"), P(None, "ba"), P(), P(), P()),
        check_vma=False,
    )
```

```python
import math

import jax
import jax.numpy as jnp
from jax import lax
from jax.experimental import pallas as pl
from jax.experimental.pallas import tpu as pltpu
from jax.sharding import Mesh
from jax.sharding import PartitionSpec as P

WIN = 8
TOKENS = WIN * WIN
LANES = 128
EPS_NORM = 1e-05
MASK_FILL = -100.0
SCALE_CAP = math.log(100.0)
BIAS_RANGE = 16.0
PROJECT_UNROLL = 4
FORWARD_UNROLL = 4
NORM_UNROLL = 4
FLATTEN_UNROLL = 4
BACKWARD_UNROLL = 4
F32 = jnp.float32
BF16 = jnp.bfloat16


def dot_nn(left, right):
    return lax.dot_general(left, right, (((1,), (0,)), ((), ())), preferred_element_type=F32)


def dot_nt(left, right):
    return lax.dot_general(left, right, (((1,), (1,)), ((), ())), preferred_element_type=F32)


def dot_tn(left, right):
    return lax.dot_general(left, right, (((0,), (0,)), ((), ())), preferred_element_type=F32)


def iota(shape, dim):
    return lax.broadcasted_iota(jnp.int32, shape, dim)


def split(value):
    high = value.astype(BF16)
    return high, (value - high.astype(F32)).astype(BF16)


def group_sum(value, ones, fine=True):
    high, low = split(value)
    width = ones.shape[0]
    parts = []
    for start in range(0, value.shape[1], width):
        part = slice(start, start + width)
        total = dot_nn(high[:, part], ones)
        parts.append(total + dot_nn(low[:, part], ones) if fine else total)
    return jnp.concatenate(parts, axis=1)


def table_maps(span, used):
    entry = iota((used, LANES), 0)
    lane = iota((used, LANES), 1)
    same_row = entry // span == lane // WIN
    near = jnp.logical_and(same_row, entry % span == lane % WIN)
    far = jnp.logical_and(same_row, entry % span == lane % WIN + WIN)
    return near.astype(F32).astype(BF16), far.astype(F32).astype(BF16)


def make_kernel(rows, cols, depth, heads, sent_rows):
    head_dim = depth // heads
    per_tile = LANES // head_dim
    groups = heads // per_tile
    col_windows = cols // WIN
    row_windows = rows // WIN
    pairs = row_windows * col_windows // 2
    pairs_across = col_windows // 2
    stacked = per_tile * TOKENS
    pair = 2 * TOKENS
    tokens = rows * cols
    span = 2 * WIN - 1
    half_q = 3 * depth // 2
    half_p = depth // 2
    body = half_q + half_p
    small_at = groups * body
    small_rows = sent_rows - small_at
    core_rows = sent_rows // 2

    def kernel(
        limit,
        img,
        w_qkv,
        w_proj,
        logits,
        gain,
        d_img,
        mine,
        given,
        xb,
        uf,
        unit_s,
        inv,
        q_low,
        q_turn,
        k_hi,
        k_lo,
        val,
        prob,
        raw,
        att,
        d_prj,
        d_att,
        d_qkv,
        d_unit,
        bias,
        d_bias,
        d_sc,
        small,
        sums,
        padded,
    ):
        core = lax.axis_index("hc")
        down = lax.axis_index("hz") * lax.axis_size("hc") + core
        last_row = (down == lax.axis_size("hz") * lax.axis_size("hc") - 1).astype(jnp.int32)
        last_col = (lax.axis_index("wa") == lax.axis_size("wa") - 1).astype(jnp.int32)
        half = iota((1, LANES), 1) < TOKENS
        wide = 2 * LANES
        ones = (iota((wide, wide), 0) // head_dim == iota((wide, wide), 1) // head_dim).astype(F32)
        ones = ones.astype(BF16)
        owner = iota((1, wide), 1) % LANES // head_dim
        head_f32 = [(owner == h).astype(F32) for h in range(per_tile)]
        head_low = [m.astype(BF16) for m in head_f32]
        top_rows = (iota((pair, LANES), 0) < TOKENS).astype(F32)
        top_rows, low_rows = top_rows.astype(BF16), (1.0 - top_rows).astype(BF16)
        left_lanes = half.astype(F32)
        left_lanes, right_lanes = left_lanes.astype(BF16), (1.0 - left_lanes).astype(BF16)
        by_head = iota((1, depth), 1) // head_dim
        scale = jnp.zeros((1, depth), F32)
        for h in range(heads):
            scale = jnp.where(by_head == h, limit[h], scale)
        scale = jnp.exp(jnp.minimum(scale, SCALE_CAP))

        def project(p, carry):
            place = pl.ds(pl.multiple_of(p * pair, pair), pair)
            pieces, ups = [], []
            for w in range(2):
                i0 = p // pairs_across * WIN
                j0 = pl.multiple_of((p % pairs_across * 2 + w) * WIN, WIN)
                for r in range(WIN):
                    pieces.append(img[0, i0 + r, pl.ds(j0, WIN), :].astype(F32))
                    ups.append(img[1, i0 + r, pl.ds(j0, WIN), :].astype(F32))
            x = jnp.concatenate(pieces, axis=0).astype(BF16)
            uf[place, :] = jnp.concatenate(ups, axis=0)
            xb[place, :] = x
            qkv = dot_nn(x, w_qkv[...]).astype(BF16)
            val[place, :] = qkv[:, 2 * depth :]
            both = qkv[:, : 2 * depth].astype(F32)
            root = lax.rsqrt(group_sum(both * both, ones) + 1.0)
            unit = both * root
            unit_s[place, :] = unit
            inv[place, :] = root[:, depth:]
            q_low[place, :] = qkv[:, :depth]
            q_turn[p] = (root[:, :depth] * scale).T
            k_hi[place, :], k_lo[place, :] = split(unit[:, depth:])
            return carry

        lax.fori_loop(0, pairs, project, 0, unroll=PROJECT_UNROLL)

        sub = iota((WIN, LANES), 0)
        lane = iota((WIN, LANES), 1)
        near_map, far_map = table_maps(span, 2 * LANES)
        padded[...] = jnp.zeros_like(padded)
        padded[:heads, : span * span] = jax.nn.sigmoid(logits[...]) * BIAS_RANGE
        table = padded[...]
        first = table.astype(BF16)
        second, third = split(table - first.astype(F32))
        table_a = dot_nn(first, near_map) + (dot_nn(second, near_map) + dot_nn(third, near_map))
        table_b = dot_nn(first, far_map) + (dot_nn(second, far_map) + dot_nn(third, far_map))
        for h in range(heads):
            near = jnp.broadcast_to(table_a[h : h + 1, :], (WIN, LANES))
            far = jnp.broadcast_to(table_b[h : h + 1, :], (WIN, LANES))
            near = pltpu.roll(near, LANES - WIN + 1, 1, stride=1, stride_axis=0)
            far = pltpu.roll(far, 1, 1, stride=1, stride_axis=0)
            line = jnp.where(lane % WIN <= sub, near, far)
            for r in range(WIN):
                one = pltpu.roll(line, (LANES - (WIN - 1 - r) * WIN) % LANES, 1)
                two = pltpu.roll(line, (LANES + TOKENS - (WIN - 1 - r) * WIN) % LANES, 1)
                at = h * TOKENS + r * WIN
                bias[at : at + WIN, :] = jnp.where(half, one, two)
        d_bias[...] = jnp.zeros_like(d_bias)
        d_sc[...] = jnp.zeros_like(d_sc)

        key = iota((TOKENS, LANES), 0)
        query = iota((TOKENS, LANES), 1) % TOKENS
        edge = WIN // 2
        split_r = ((key // WIN) >= edge) != ((query // WIN) >= edge)
        split_c = ((key % WIN) >= edge) != ((query % WIN) >= edge)
        split_c = jnp.logical_and(split_c, iota((TOKENS, LANES), 1) >= TOKENS)
        mask_r = jnp.where(split_r, MASK_FILL, 0.0)
        mask_c = jnp.where(split_c, MASK_FILL, 0.0)

        def beside(ref, at, tile):
            one = ref[pl.ds(at, TOKENS), tile]
            two = ref[pl.ds(at + TOKENS, TOKENS), tile]
            return jnp.concatenate([one, two], axis=1)

        def stack(block):
            return jnp.concatenate([block * head_low[h] for h in range(per_tile)], axis=0)

        def diagonal(ref, at, tile):
            block = ref[pl.ds(at, pair), tile]
            return jnp.concatenate([block * top_rows, block * low_rows], axis=1)

        def turned(ref, at, tile):
            block = ref[pl.ds(at, pair), tile].T
            return jnp.concatenate([block * left_lanes, block * right_lanes], axis=0)

        def gather_heads(out):
            total = out[:TOKENS] * head_f32[0]
            for h in range(1, per_tile):
                total = total + out[h * TOKENS : (h + 1) * TOKENS] * head_f32[h]
            return total

        def forward(p, carry):
            at = pl.multiple_of(p * pair, pair)
            row_edge = jnp.where(p // pairs_across == row_windows - 1, last_row, 0)
            col_edge = jnp.where(p % pairs_across == pairs_across - 1, last_col, 0)
            mask = jnp.minimum(mask_r * row_edge.astype(F32), mask_c * col_edge.astype(F32))
            for g in range(groups):
                tile = slice(g * LANES, (g + 1) * LANES)
                keys = stack(beside(k_hi, at, tile))
                keys_low = stack(beside(k_lo, at, tile))
                queries = turned(q_low, at, tile)
                score = dot_nn(keys, queries) + dot_nn(keys_low, queries)
                lows = []
                for h in range(per_tile):
                    place = slice(h * TOKENS, (h + 1) * TOKENS)
                    of = (g * per_tile + h) * TOKENS
                    line = (g * per_tile + h) * head_dim
                    s = score[place] * q_turn[p, line : line + 1, :]
                    raw[p, g, place, :] = s
                    s = s + (bias[of : of + TOKENS, :] + mask)
                    e = jnp.exp(s - jnp.max(s, axis=0, keepdims=True))
                    pr = e * (1.0 / jnp.sum(e, axis=0, keepdims=True))
                    prob[p, g, place, :] = pr
                    lows.append(pr.astype(BF16))
                out = dot_tn(jnp.concatenate(lows, axis=0), stack(beside(val, at, tile)))
                att[pl.ds(at, TOKENS), tile] = out[:TOKENS, :LANES].astype(BF16)
                att[pl.ds(at + TOKENS, TOKENS), tile] = out[TOKENS:, LANES:].astype(BF16)
            return carry

        lax.fori_loop(0, pairs, forward, 0, unroll=FORWARD_UNROLL)

        gains = gain[...].reshape(1, depth)

        def norm(p, d_gain):
            place = pl.ds(pl.multiple_of(p * pair, pair), pair)
            proj = dot_nn(att[place, :], w_proj[...])
            centre = proj - jnp.mean(proj, -1, keepdims=True)
            std = lax.rsqrt(jnp.mean(centre * centre, -1, keepdims=True) + EPS_NORM)
            normed = centre * std
            up = uf[place, :]
            d_gain = d_gain + jnp.sum(up * normed, axis=0, keepdims=True)
            u = up * gains
            d_p = std * (
                u - jnp.mean(u, -1, keepdims=True) - normed * jnp.mean(u * normed, -1, keepdims=True)
            )
            d_p = d_p.astype(BF16)
            d_prj[place, :] = d_p
            return d_gain

        d_gain = lax.fori_loop(0, pairs, norm, jnp.zeros((1, depth), F32), unroll=NORM_UNROLL)

        w_proj_turned = w_proj[...].T

        def spread(p, carry):
            place = pl.ds(pl.multiple_of(p * pair, pair), pair)
            d_att[place, :] = dot_nn(d_prj[place, :], w_proj_turned).astype(BF16)
            return carry

        lax.fori_loop(0, pairs, spread, 0, unroll=NORM_UNROLL)

        def backward(p, carry):
            at = pl.multiple_of(p * pair, pair)
            for g in range(groups):
                tile = slice(g * LANES, (g + 1) * LANES)
                key_tile = slice(depth + g * LANES, depth + (g + 1) * LANES)
                val_tile = slice(2 * depth + g * LANES, 2 * depth + (g + 1) * LANES)
                values = stack(beside(val, at, tile))
                ups = diagonal(d_att, at, tile)
                d_pr = dot_nn(values, turned(d_att, at, tile))
                lows, d_lows = [], []
                for h in range(per_tile):
                    place = slice(h * TOKENS, (h + 1) * TOKENS)
                    of = (g * per_tile + h) * TOKENS
                    pr = prob[p, g, place, :]
                    pd = pr * d_pr[place]
                    d_s = pd - pr * jnp.sum(pd, axis=0, keepdims=True)
                    d_bias[of : of + TOKENS, :] += d_s
                    by_scale = (d_s * raw[p, g, place, :]).reshape(WIN, WIN, LANES)
                    head = g * per_tile + h
                    d_sc[head * WIN : (head + 1) * WIN, :] += jnp.sum(by_scale, axis=0)
                    lows.append(pr.astype(BF16))
                    line = head * head_dim
                    d_lows.append((d_s * q_turn[p, line : line + 1, :]).astype(BF16))
                low = jnp.concatenate(lows, axis=0)
                d_low = jnp.concatenate(d_lows, axis=0)
                d_v = gather_heads(dot_nn(low, ups)).astype(BF16)
                d_qkv[pl.ds(at, TOKENS), val_tile] = d_v[:, :LANES]
                d_qkv[pl.ds(at + TOKENS, TOKENS), val_tile] = d_v[:, LANES:]
                d_k = gather_heads(dot_nn(d_low, diagonal(q_low, at, tile)))
                d_unit[pl.ds(at, TOKENS), key_tile] = d_k[:, :LANES]
                d_unit[pl.ds(at + TOKENS, TOKENS), key_tile] = d_k[:, LANES:]
                d_q = dot_tn(d_low, stack(beside(k_hi, at, tile)))
                d_unit[pl.ds(at, TOKENS), tile] = d_q[:TOKENS, :LANES]
                d_unit[pl.ds(at + TOKENS, TOKENS), tile] = d_q[TOKENS:, LANES:]
            return carry

        lax.fori_loop(0, pairs, backward, 0, unroll=BACKWARD_UNROLL)

        w_qkv_turned = w_qkv[...].T

        def flatten(p, carry):
            place = pl.ds(pl.multiple_of(p * pair, pair), pair)
            unit = unit_s[place, :]
            d_u = d_unit[place, :]
            d_u = d_u - unit * group_sum(unit * d_u, ones, False)
            d_qkv[place, :depth] = d_u[:, :depth].astype(BF16)
            d_qkv[place, depth : 2 * depth] = (inv[place, :] * d_u[:, depth:]).astype(BF16)
            flat = dot_nn(d_qkv[place, :], w_qkv_turned)
            for w in range(2):
                i0 = p // pairs_across * WIN
                j0 = pl.multiple_of((p % pairs_across * 2 + w) * WIN, WIN)
                for r in range(WIN):
                    piece = flat[w * TOKENS + r * WIN : w * TOKENS + (r + 1) * WIN]
                    d_img[i0 + r, pl.ds(j0, WIN), :] = piece.astype(BF16)
            return carry

        lax.fori_loop(0, pairs, flatten, 0, unroll=FLATTEN_UNROLL)

        d_wp = dot_tn(d_prj[...], att[...])
        d_wq = dot_tn(d_qkv[...], xb[...])
        for b in range(2):
            for j in range(groups):
                tile = slice(j * LANES, (j + 1) * LANES)
                at = j * body
                sums[b, at : at + half_q, :] = d_wq[b * half_q : (b + 1) * half_q, tile].astype(BF16)
                at = at + half_q
                sums[b, at : at + half_p, :] = d_wp[b * half_p : (b + 1) * half_p, tile].astype(BF16)

        small[...] = jnp.zeros_like(small)
        for h in range(heads):
            line = jnp.zeros((WIN, LANES), F32)
            for r in range(WIN):
                at = h * TOKENS + r * WIN
                part = d_bias[at : at + WIN, :]
                part = jnp.where(half, part + pltpu.roll(part, TOKENS, 1), 0.0)
                line = line + pltpu.roll(part, (WIN - 1 - r) * WIN, 1)
            near, far = jnp.zeros_like(line), jnp.zeros_like(line)
            for c in range(WIN):
                own = jnp.where(sub == c, line, 0.0)
                near = near + pltpu.roll(own, WIN - 1 - c, 1)
                far = far + pltpu.roll(own, LANES - 1 - c, 1)
            near = jnp.where(lane % WIN >= WIN - 1 - sub, near, 0.0)
            far = jnp.where(lane % WIN + sub + 1 <= WIN - 1, far, 0.0)
            small[h : h + 1, :] = jnp.sum(near, axis=0, keepdims=True)
            small[heads + h : heads + h + 1, :] = jnp.sum(far, axis=0, keepdims=True)
        for j in range(groups):
            small[2 * heads + j : 2 * heads + j + 1, :] = d_gain[:, j * LANES : (j + 1) * LANES]
        line = jnp.zeros((1, LANES), F32)
        for h in range(heads):
            total = jnp.sum(d_sc[h * WIN : (h + 1) * WIN, :], axis=0, keepdims=True)
            total = jnp.sum(total, axis=1, keepdims=True)
            line = line + jnp.where(iota((1, LANES), 1) == h, total, 0.0)
        at = 2 * heads + groups
        small[at : at + 1, :] = line
        for b in range(2):
            sums[b, small_at:, :] = small[...].astype(BF16)
        own = pl.multiple_of(core * core_rows, 8)
        other = pl.multiple_of((1 - core) * core_rows, 8)
        for b in range(2):
            mine[b] = sums[b, pl.ds(own, core_rows), :]
            given[b] = sums[b, pl.ds(other, core_rows), :]

    def call(limit, img, w_qkv, w_proj, logits, gain):
        vmem = pltpu.VMEM
        scratch = [
            vmem((tokens, depth), BF16),
            vmem((tokens, depth), F32),
            vmem((tokens, 2 * depth), F32),
            vmem((tokens, depth), F32),
            vmem((tokens, depth), BF16),
            vmem((pairs, depth, pair), F32),
            vmem((tokens, depth), BF16),
            vmem((tokens, depth), BF16),
            vmem((tokens, depth), BF16),
            vmem((pairs, groups, stacked, LANES), F32),
            vmem((pairs, groups, stacked, LANES), F32),
            vmem((tokens, depth), BF16),
            vmem((tokens, depth), BF16),
            vmem((tokens, depth), BF16),
            vmem((tokens, 3 * depth), BF16),
            vmem((tokens, 2 * depth), F32),
            vmem((heads * TOKENS, LANES), F32),
            vmem((heads * TOKENS, LANES), F32),
            vmem((heads * WIN, LANES), F32),
            vmem((small_rows, LANES), F32),
            vmem((2, sent_rows, LANES), BF16),
            vmem((16, 2 * LANES), F32),
        ]
        part = jax.ShapeDtypeStruct((2, core_rows, LANES), BF16)
        return pl.pallas_call(
            kernel,
            out_shape=(jax.ShapeDtypeStruct((rows, cols, depth), BF16), part, part),
            in_specs=[pl.BlockSpec(memory_space=pltpu.SMEM)]
            + [pl.BlockSpec(memory_space=pltpu.VMEM)] * 5,
            out_specs=tuple([pl.BlockSpec(memory_space=pltpu.VMEM)] * 3),
            scratch_shapes=scratch,
            name="block_grads",
        )(limit, img, w_qkv, w_proj, logits, gain)

    return call


def finish(ours, theirs, logits, limit, depth, heads):
    core_rows = ours.shape[0]
    groups = depth // LANES
    half_q = 3 * depth // 2
    half_p = depth // 2
    body = half_q + half_p
    small_at = groups * body
    span = 2 * WIN - 1

    def kernel(limit, ours, theirs, logits, d_wq, d_wp, d_table, d_scale, d_gain, whole):
        core = lax.axis_index("hc")
        whole[pl.ds(pl.multiple_of(core * core_rows, 8), core_rows), :] = ours[...].astype(F32)
        other = pl.multiple_of((1 - core) * core_rows, 8)
        whole[pl.ds(other, core_rows), :] = theirs[...].astype(F32)
        for j in range(groups):
            tile = slice(j * LANES, (j + 1) * LANES)
            d_wq[:, tile] = whole[j * body : j * body + half_q, :]
            d_wp[:, tile] = whole[j * body + half_q : (j + 1) * body, :]
        small = whole[small_at : small_at + 32, :]
        near_map, far_map = table_maps(span, 2 * LANES)
        table = dot_nt(small[:16].astype(BF16), near_map)
        table = table + dot_nt(small[heads : heads + 16].astype(BF16), far_map)
        table = table[:heads, : span * span]
        sigma = jax.nn.sigmoid(logits[...])
        d_table[...] = table * (BIAS_RANGE * sigma * (1.0 - sigma))
        gains = [small[2 * heads + j : 2 * heads + j + 1, :] for j in range(groups)]
        d_gain[...] = jnp.concatenate(gains, axis=1).reshape(depth)
        lane = iota((1, LANES), 1)
        kept = jnp.zeros((1, LANES), F32)
        for h in range(heads):
            kept = jnp.where(lane == h, jnp.where(limit[h] < SCALE_CAP, 1.0, 0.0), kept)
        row = small[2 * heads + groups : 2 * heads + groups + 1, :] * kept
        d_scale[...] = row[:, :heads].reshape(heads)

    vmem = pl.BlockSpec(memory_space=pltpu.VMEM)
    return pl.pallas_call(
        kernel,
        out_shape=(
            jax.ShapeDtypeStruct((half_q, depth), F32),
            jax.ShapeDtypeStruct((half_p, depth), F32),
            jax.ShapeDtypeStruct(logits.shape, F32),
            jax.ShapeDtypeStruct((heads,), F32),
            jax.ShapeDtypeStruct((depth,), F32),
        ),
        in_specs=[pl.BlockSpec(memory_space=pltpu.SMEM), vmem, vmem, vmem],
        out_specs=(vmem,) * 5,
        scratch_shapes=[pltpu.VMEM((2 * core_rows, LANES), F32)],
        name="finish",
    )(limit, ours, theirs, logits)


def route(axes, move):
    sizes = [lax.axis_size(a) for a in axes]
    pairs = []
    for flat in range(math.prod(sizes)):
        left, where = flat, []
        for size in reversed(sizes):
            where.append(left % size)
            left //= size
        where = move(where[::-1], sizes)
        target = 0
        for place, size in zip(where, sizes):
            target = target * size + place
        pairs.append((flat, target))
    return pairs


GRID = ("hz", "hc", "wa")


def step(rows, cols):
    def move(where, sizes):
        high = (where[0] * sizes[1] + where[1] + rows) % (sizes[0] * sizes[1])
        return [high // sizes[1], high % sizes[1], (where[2] + cols) % sizes[2]]

    return move


def shards(tokens, cotangent, w_qkv, w_proj, table_logits, logit_scale, gain):
    images, rows, cols, depth = tokens.shape
    heads = logit_scale.shape[0]
    edge = WIN // 2
    both = jnp.concatenate([tokens, cotangent], 0)
    below = lax.ppermute(both[:, :edge], GRID, route(GRID, step(-1, 0)))
    beside = lax.ppermute(both[:, :, :edge], GRID, route(GRID, step(0, -1)))
    corner = lax.ppermute(both[:, :edge, :edge], GRID, route(GRID, step(-1, -1)))
    main = jnp.concatenate([both[:, edge:, edge:], beside[:, edge:]], 2)
    last = jnp.concatenate([below[:, :, edge:], corner], 2)
    moved = jnp.concatenate([main, last], 1)

    cores, tall, across = lax.axis_size("hc"), lax.axis_size("hz"), lax.axis_size("wa")
    owners = cores * tall * across
    used = 2 * depth // LANES * depth + 2 * heads + depth // LANES + 1
    unit = 8 * owners
    sent = -(-used // unit) * unit
    call = make_kernel(rows, cols, depth, heads, sent)
    d_moved, mine, given = call(logit_scale, moved, w_qkv, w_proj, table_logits, gain)

    right = lax.ppermute(d_moved[: rows - edge, cols - edge :], GRID, route(GRID, step(0, 1)))
    lower = lax.ppermute(d_moved[rows - edge :, : cols - edge], GRID, route(GRID, step(1, 0)))
    cross = lax.ppermute(
        d_moved[rows - edge :, cols - edge :], GRID, route(GRID, step(1, 1))
    )
    upper = jnp.concatenate([cross, lower], 1)
    main = jnp.concatenate([right, d_moved[: rows - edge, : cols - edge]], 1)
    back = jnp.concatenate([upper, main], 0)[None]
    d_tokens = (cotangent.astype(F32) + back.astype(F32)).astype(BF16)

    swap = route(("hc",), lambda where, sizes: [1 - where[0]])
    taken = lax.ppermute(given, "hc", swap)
    summed = (mine.astype(F32) + taken.astype(F32)).astype(BF16)
    piece = sent // owners
    summed = summed.reshape(2 * tall * across, piece, LANES)
    parts = lax.all_to_all(summed, ("ba", "hz", "wa"), 0, 0, tiled=True)
    total = parts.astype(F32).sum(0).astype(BF16)
    spread = jnp.broadcast_to(total[None], (tall * across, piece, LANES))
    ours = lax.all_to_all(spread, ("hz", "wa"), 0, 0, tiled=True)
    ours = ours.reshape(sent // cores, LANES)
    theirs = lax.ppermute(ours, "hc", swap)
    d_wq, d_wp, d_table, d_scale, d_gain = finish(
        ours, theirs, table_logits, logit_scale, depth, heads
    )
    return (d_tokens, d_wq.T, d_wp.T, d_table, d_scale, d_gain)


def solution(mesh):
    sizes = mesh.shape
    devices = mesh.devices.reshape(sizes["ha"] // 2, 2, sizes["wa"], sizes["ba"])
    inner = Mesh(devices, ("hz", "hc", "wa", "ba"))
    image = P("ba", ("hz", "hc"), "wa", None)
    return jax.shard_map(
        shards,
        mesh=inner,
        in_specs=(image, image, P(), P(), P(), P(), P()),
        out_specs=(image, P(None, "ba"), P(None, "ba"), P(), P(), P()),
        check_vma=False,
    )
```

```python
import functools
import math

import jax
import jax.numpy as jnp
from jax import lax
from jax.experimental import pallas as pl
from jax.experimental.pallas import tpu as pltpu
from jax.sharding import Mesh
from jax.sharding import PartitionSpec as P

WIN = 8
TOKENS = WIN * WIN
LANES = 128
EPS_NORM = 1e-05
MASK_FILL = -100.0
SCALE_CAP = math.log(100.0)
BIAS_RANGE = 16.0
LOG2_E = math.log2(math.e)
VMEM_MAIN = 36 << 20
VMEM_LAST = 12 << 20
F32 = jnp.float32
BF16 = jnp.bfloat16


def dot_nn(left, right):
    return lax.dot_general(left, right, (((1,), (0,)), ((), ())), preferred_element_type=F32)


def dot_nt(left, right):
    return lax.dot_general(left, right, (((1,), (1,)), ((), ())), preferred_element_type=F32)


def dot_tn(left, right):
    return lax.dot_general(left, right, (((0,), (0,)), ((), ())), preferred_element_type=F32)


def iota(shape, dim):
    return lax.broadcasted_iota(jnp.int32, shape, dim)


def split(value):
    high = value.astype(BF16)
    return high, (value - high.astype(F32)).astype(BF16)


def group_sum(value, ones, fine=True):
    high, low = split(value)
    width = ones.shape[0]
    parts = []
    for start in range(0, value.shape[1], width):
        part = slice(start, start + width)
        total = dot_nn(high[:, part], ones)
        parts.append(total + dot_nn(low[:, part], ones) if fine else total)
    return jnp.concatenate(parts, axis=1)


def table_maps(span, used):
    entry = iota((used, LANES), 0)
    lane = iota((used, LANES), 1)
    same_row = entry // span == lane // WIN
    near = jnp.logical_and(same_row, entry % span == lane % WIN)
    far = jnp.logical_and(same_row, entry % span == lane % WIN + WIN)
    return near.astype(F32).astype(BF16), far.astype(F32).astype(BF16)


def repeat(count, step, carry=0):
    for p in range(count):
        carry = step(p, carry)
    return carry


def pipeline(items, stages):
    for start in range(len(items) + len(stages) - 1):
        for back, stage in enumerate(stages):
            if 0 <= start - back < len(items):
                stage(*items[start - back])


def make_kernel(rows, cols, depth, heads, sent_rows, across, order):
    head_dim = depth // heads
    per_tile = LANES // head_dim
    groups = heads // per_tile
    col_windows = cols // WIN
    row_windows = rows // WIN
    pairs = row_windows * col_windows // 2
    pairs_across = col_windows // 2
    stacked = per_tile * TOKENS
    pair = 2 * TOKENS
    tokens = rows * cols
    span = 2 * WIN - 1
    half_q = 3 * depth // 2
    half_p = depth // 2
    body = half_q + half_p
    small_at = groups * body
    small_rows = sent_rows - small_at
    core_rows = sent_rows // 2
    edge = WIN // 2
    pitch = cols + WIN
    outer, inner, crossed = order
    chunk = core_rows // across

    def kernel(
        limit,
        tok,
        cot,
        below,
        right,
        corner,
        w_qkv,
        w_proj,
        logits,
        gain,
        d_img,
        mine,
        given,
        xb,
        uf,
        unit_s,
        inv,
        q_low,
        q_turn,
        k_hi,
        k_lo,
        val,
        prob,
        prob_low,
        raw,
        d_prob,
        d_low,
        att,
        d_prj,
        d_att,
        d_qkv,
        d_unit,
        bias,
        d_bias,
        d_sc,
        small,
        sums,
        padded,
        wide_x,
        wide_u,
    ):
        core = lax.axis_index("hc")
        down = lax.axis_index("hz") * lax.axis_size("hc") + core
        last_row = (down == lax.axis_size("hz") * lax.axis_size("hc") - 1).astype(jnp.int32)
        last_col = (lax.axis_index("wa") == lax.axis_size("wa") - 1).astype(jnp.int32)
        half = iota((1, LANES), 1) < TOKENS
        wide = 2 * LANES
        ones = (iota((wide, wide), 0) // head_dim == iota((wide, wide), 1) // head_dim).astype(F32)
        ones = ones.astype(BF16)
        owner = iota((1, wide), 1) % LANES // head_dim
        head_low = [(owner == h).astype(F32).astype(BF16) for h in range(per_tile)]
        top_rows = (iota((pair, LANES), 0) < TOKENS).astype(F32)
        top_rows, low_rows = top_rows.astype(BF16), (1.0 - top_rows).astype(BF16)
        left_lanes = half.astype(F32)
        left_lanes, right_lanes = left_lanes.astype(BF16), (1.0 - left_lanes).astype(BF16)
        by_head = iota((1, depth), 1) // head_dim
        scale = jnp.zeros((1, depth), F32)
        for h in range(heads):
            scale = jnp.where(by_head == h, limit[h], scale)
        scale = jnp.exp(jnp.minimum(scale, SCALE_CAP))

        for which, (own, wide_of) in enumerate(((tok, wide_x), (cot, wide_u))):
            edges = right[which].astype(F32)
            ends = corner[which].astype(F32)
            for i in range(rows):
                if i + edge < rows:
                    row = own[0, i + edge].astype(F32)
                    side = edges[(i + edge) * edge : (i + edge + 1) * edge]
                else:
                    row = below[which, i + edge - rows].astype(F32)
                    side = ends[(i + edge - rows) * edge : (i + edge - rows + 1) * edge]
                at = i * pitch
                for j in range(groups):
                    tile = slice(j * LANES, (j + 1) * LANES)
                    wide_of[j, at : at + cols, :] = row[:, tile]
                    wide_of[j, at + cols : at + cols + edge, :] = side[:, tile]

        def window_rows(wide_of, p):
            tiles = []
            for j in range(groups):
                pieces = []
                for w in range(2):
                    i0 = p // pairs_across * WIN
                    j0 = (p % pairs_across * 2 + w) * WIN + edge
                    for r in range(WIN):
                        at = (i0 + r) * pitch + j0
                        pieces.append(wide_of[j, at : at + WIN, :])
                tiles.append(jnp.concatenate(pieces, axis=0))
            return jnp.concatenate(tiles, axis=1)

        def project(p, carry):
            place = pl.ds(p * pair, pair)
            x = window_rows(wide_x, p).astype(BF16)
            uf[place, :] = window_rows(wide_u, p)
            xb[place, :] = x
            qkv = dot_nn(x, w_qkv[...]).astype(BF16)
            val[place, :] = qkv[:, 2 * depth :]
            both = qkv[:, : 2 * depth].astype(F32)
            root = lax.rsqrt(group_sum(both * both, ones) + 1.0)
            unit = both * root
            unit_s[place, :] = unit
            inv[place, :] = root[:, depth:]
            q_low[place, :] = qkv[:, :depth]
            q_turn[p] = (root[:, :depth] * scale).T
            k_hi[place, :], k_lo[place, :] = split(unit[:, depth:])
            return carry

        repeat(pairs, project)

        sub = iota((WIN, LANES), 0)
        lane = iota((WIN, LANES), 1)
        near_map, far_map = table_maps(span, 2 * LANES)
        padded[...] = jnp.zeros_like(padded)
        padded[:heads, : span * span] = jax.nn.sigmoid(logits[...]) * (BIAS_RANGE * LOG2_E)
        table = padded[...]
        first = table.astype(BF16)
        second, third = split(table - first.astype(F32))
        table_a = dot_nn(first, near_map) + (dot_nn(second, near_map) + dot_nn(third, near_map))
        table_b = dot_nn(first, far_map) + (dot_nn(second, far_map) + dot_nn(third, far_map))
        for h in range(heads):
            near = jnp.broadcast_to(table_a[h : h + 1, :], (WIN, LANES))
            far = jnp.broadcast_to(table_b[h : h + 1, :], (WIN, LANES))
            near = pltpu.roll(near, LANES - WIN + 1, 1, stride=1, stride_axis=0)
            far = pltpu.roll(far, 1, 1, stride=1, stride_axis=0)
            line = jnp.where(lane % WIN <= sub, near, far)
            for r in range(WIN):
                one = pltpu.roll(line, (LANES - (WIN - 1 - r) * WIN) % LANES, 1)
                two = pltpu.roll(line, (LANES + TOKENS - (WIN - 1 - r) * WIN) % LANES, 1)
                at = h * TOKENS + r * WIN
                bias[at : at + WIN, :] = jnp.where(half, one, two)

        key = iota((TOKENS, LANES), 0)
        query = iota((TOKENS, LANES), 1) % TOKENS
        split_r = ((key // WIN) >= edge) != ((query // WIN) >= edge)
        split_c = ((key % WIN) >= edge) != ((query % WIN) >= edge)
        split_c = jnp.logical_and(split_c, iota((TOKENS, LANES), 1) >= TOKENS)
        mask_r = jnp.where(split_r, MASK_FILL * LOG2_E, 0.0)
        mask_c = jnp.where(split_c, MASK_FILL * LOG2_E, 0.0)

        def beside(ref, at, tile):
            one = ref[pl.ds(at, TOKENS), tile]
            two = ref[pl.ds(at + TOKENS, TOKENS), tile]
            return jnp.concatenate([one, two], axis=1)

        def stack(block):
            return jnp.concatenate([block * head_low[h] for h in range(per_tile)], axis=0)

        def diagonal(ref, at, tile):
            block = ref[pl.ds(at, pair), tile]
            return jnp.concatenate([block * top_rows, block * low_rows], axis=1)

        def turned(ref, at, tile):
            block = ref[pl.ds(at, pair), tile].T
            return jnp.concatenate([block * left_lanes, block * right_lanes], axis=0)

        def gather_heads(out):
            total = out[:TOKENS]
            for h in range(1, per_tile):
                total = jnp.where(owner == h, out[h * TOKENS : (h + 1) * TOKENS], total)
            return total

        tiles = [(p, g) for p in range(pairs) for g in range(groups)]

        def lanes_of(g):
            return slice(g * LANES, (g + 1) * LANES)

        def score(p, g):
            keys = stack(beside(k_hi, p * pair, lanes_of(g)))
            keys_low = stack(beside(k_lo, p * pair, lanes_of(g)))
            queries = turned(q_low, p * pair, lanes_of(g))
            raw[p, g] = dot_nn(keys, queries) + dot_nn(keys_low, queries)

        def soften(p, g):
            masks = []
            if p // pairs_across == row_windows - 1:
                masks.append(mask_r * last_row.astype(F32))
            if p % pairs_across == pairs_across - 1:
                masks.append(mask_c * last_col.astype(F32))
            for h in range(per_tile):
                place = slice(h * TOKENS, (h + 1) * TOKENS)
                head = g * per_tile + h
                line = q_turn[p, head * head_dim : head * head_dim + 1, :] * LOG2_E
                added = bias[head * TOKENS : (head + 1) * TOKENS, :]
                if masks:
                    added = added + functools.reduce(jnp.minimum, masks)
                s = raw[p, g, place, :] * line + added
                e = jnp.exp2(s - jnp.max(s, axis=0, keepdims=True))
                pr = e * (1.0 / jnp.sum(e, axis=0, keepdims=True))
                prob[p, g, place, :] = pr
                prob_low[p, g, place, :] = pr.astype(BF16)

        def attend(p, g):
            at, tile = p * pair, lanes_of(g)
            out = dot_tn(prob_low[p, g], stack(beside(val, at, tile)))
            att[at : at + TOKENS, tile] = out[:TOKENS, :LANES].astype(BF16)
            att[at + TOKENS : at + pair, tile] = out[TOKENS:, LANES:].astype(BF16)

        pipeline(tiles, (score, soften, attend))

        gains = gain[...].reshape(1, depth)

        def norm(p, d_gain):
            place = pl.ds(p * pair, pair)
            proj = dot_nn(att[place, :], w_proj[...])
            centre = proj - jnp.mean(proj, -1, keepdims=True)
            std = lax.rsqrt(jnp.mean(centre * centre, -1, keepdims=True) + EPS_NORM)
            normed = centre * std
            up = uf[place, :]
            d_gain = d_gain + jnp.sum(up * normed, axis=0, keepdims=True)
            u = up * gains
            d_p = std * (
                u - jnp.mean(u, -1, keepdims=True) - normed * jnp.mean(u * normed, -1, keepdims=True)
            )
            d_p = d_p.astype(BF16)
            d_prj[place, :] = d_p
            return d_gain

        d_gain = repeat(pairs, norm, jnp.zeros((1, depth), F32))

        w_proj_turned = w_proj[...].T

        def spread(p, carry):
            place = pl.ds(p * pair, pair)
            d_att[place, :] = dot_nn(d_prj[place, :], w_proj_turned).astype(BF16)
            return carry

        repeat(pairs, spread)

        def rise(p, g):
            values = stack(beside(val, p * pair, lanes_of(g)))
            d_prob[p, g] = dot_nn(values, turned(d_att, p * pair, lanes_of(g)))

        def harden(p, g):
            for h in range(per_tile):
                place = slice(h * TOKENS, (h + 1) * TOKENS)
                head = g * per_tile + h
                of = slice(head * TOKENS, (head + 1) * TOKENS)
                pr = prob[p, g, place, :]
                pd = pr * d_prob[p, g, place, :]
                d_s = pd - pr * jnp.sum(pd, axis=0, keepdims=True)
                if p == 0:
                    d_bias[of, :] = d_s
                else:
                    d_bias[of, :] += d_s
                d_s = d_s * q_turn[p, head * head_dim : head * head_dim + 1, :]
                by_scale = (d_s * raw[p, g, place, :]).reshape(WIN, WIN, LANES)
                of = slice(head * WIN, (head + 1) * WIN)
                if p == 0:
                    d_sc[of, :] = jnp.sum(by_scale, axis=0)
                else:
                    d_sc[of, :] += jnp.sum(by_scale, axis=0)
                d_low[p, g, place, :] = d_s.astype(BF16)

        def fall(p, g):
            at, tile = p * pair, lanes_of(g)
            key_tile = slice(depth + g * LANES, depth + (g + 1) * LANES)
            val_tile = slice(2 * depth + g * LANES, 2 * depth + (g + 1) * LANES)
            d_v = gather_heads(dot_nn(prob_low[p, g], diagonal(d_att, at, tile))).astype(BF16)
            d_qkv[at : at + TOKENS, val_tile] = d_v[:, :LANES]
            d_qkv[at + TOKENS : at + pair, val_tile] = d_v[:, LANES:]
            d_k = gather_heads(dot_nn(d_low[p, g], diagonal(q_low, at, tile)))
            d_unit[at : at + TOKENS, key_tile] = d_k[:, :LANES]
            d_unit[at + TOKENS : at + pair, key_tile] = d_k[:, LANES:]
            d_q = dot_tn(d_low[p, g], stack(beside(k_hi, at, tile)))
            d_unit[at : at + TOKENS, tile] = d_q[:TOKENS, :LANES]
            d_unit[at + TOKENS : at + pair, tile] = d_q[TOKENS:, LANES:]

        pipeline(tiles, (rise, harden, fall))

        w_qkv_turned = w_qkv[...].T

        def flatten(p, carry):
            place = pl.ds(p * pair, pair)
            unit = unit_s[place, :]
            d_u = d_unit[place, :]
            d_u = d_u - unit * group_sum(unit * d_u, ones, False)
            d_qkv[place, :depth] = d_u[:, :depth].astype(BF16)
            d_qkv[place, depth : 2 * depth] = (inv[place, :] * d_u[:, depth:]).astype(BF16)
            flat = dot_nn(d_qkv[place, :], w_qkv_turned)
            for w in range(2):
                i0 = p // pairs_across * WIN
                j0 = (p % pairs_across * 2 + w) * WIN
                for r in range(WIN):
                    piece = flat[w * TOKENS + r * WIN : w * TOKENS + (r + 1) * WIN]
                    d_img[i0 + r, pl.ds(j0, WIN), :] = piece.astype(BF16)
            return carry

        repeat(pairs, flatten)

        d_wp = dot_tn(d_prj[...], att[...])
        d_wq = dot_tn(d_qkv[...], xb[...])
        for b in range(2):
            for j in range(groups):
                tile = slice(j * LANES, (j + 1) * LANES)
                at = b * sent_rows + j * body
                sums[at : at + half_q, :] = d_wq[b * half_q : (b + 1) * half_q, tile].astype(BF16)
                at = at + half_q
                sums[at : at + half_p, :] = d_wp[b * half_p : (b + 1) * half_p, tile].astype(BF16)

        small[...] = jnp.zeros_like(small)
        for h in range(heads):
            line = jnp.zeros((WIN, LANES), F32)
            for r in range(WIN):
                at = h * TOKENS + r * WIN
                part = d_bias[at : at + WIN, :]
                part = jnp.where(half, part + pltpu.roll(part, TOKENS, 1), 0.0)
                line = line + pltpu.roll(part, (WIN - 1 - r) * WIN, 1)
            near, far = jnp.zeros_like(line), jnp.zeros_like(line)
            for c in range(WIN):
                own = jnp.where(sub == c, line, 0.0)
                near = near + pltpu.roll(own, WIN - 1 - c, 1)
                far = far + pltpu.roll(own, LANES - 1 - c, 1)
            near = jnp.where(lane % WIN >= WIN - 1 - sub, near, 0.0)
            far = jnp.where(lane % WIN + sub + 1 <= WIN - 1, far, 0.0)
            small[h : h + 1, :] = jnp.sum(near, axis=0, keepdims=True)
            small[heads + h : heads + h + 1, :] = jnp.sum(far, axis=0, keepdims=True)
        for j in range(groups):
            small[2 * heads + j : 2 * heads + j + 1, :] = d_gain[:, j * LANES : (j + 1) * LANES]
        line = jnp.zeros((1, LANES), F32)
        for h in range(heads):
            total = jnp.sum(d_sc[h * WIN : (h + 1) * WIN, :], axis=0, keepdims=True)
            total = jnp.sum(total, axis=1, keepdims=True)
            line = line + jnp.where(iota((1, LANES), 1) == h, total, 0.0)
        at = 2 * heads + groups
        small[at : at + 1, :] = line
        for b in range(2):
            at = b * sent_rows + small_at
            sums[at : at + small_rows, :] = small[...].astype(BF16)
        for out, whose in ((mine, core), (given, 1 - core)):
            turn = whose if crossed else 0
            for f in range(outer):
                for n in range(inner):
                    image = f + (n - f) * turn
                    column = n + (f - n) * turn
                    at = image * sent_rows + whose * core_rows + column * chunk
                    out[f, n] = sums[pl.ds(pl.multiple_of(at, 8), chunk), :]

    def call(limit, tok, cot, below, right, corner, w_qkv, w_proj, logits, gain):
        vmem = pltpu.VMEM
        scratch = [
            vmem((tokens, depth), BF16),
            vmem((tokens, depth), F32),
            vmem((tokens, 2 * depth), F32),
            vmem((tokens, depth), F32),
            vmem((tokens, depth), BF16),
            vmem((pairs, depth, pair), F32),
            vmem((tokens, depth), BF16),
            vmem((tokens, depth), BF16),
            vmem((tokens, depth), BF16),
            vmem((pairs, groups, stacked, LANES), F32),
            vmem((pairs, groups, stacked, LANES), BF16),
            vmem((pairs, groups, stacked, LANES), F32),
            vmem((pairs, groups, stacked, LANES), F32),
            vmem((pairs, groups, stacked, LANES), BF16),
            vmem((tokens, depth), BF16),
            vmem((tokens, depth), BF16),
            vmem((tokens, depth), BF16),
            vmem((tokens, 3 * depth), BF16),
            vmem((tokens, 2 * depth), F32),
            vmem((heads * TOKENS, LANES), F32),
            vmem((heads * TOKENS, LANES), F32),
            vmem((heads * WIN, LANES), F32),
            vmem((small_rows, LANES), F32),
            vmem((2 * sent_rows, LANES), BF16),
            vmem((16, 2 * LANES), F32),
            vmem((groups, rows * pitch, LANES), F32),
            vmem((groups, rows * pitch, LANES), F32),
        ]
        part = jax.ShapeDtypeStruct((outer, inner, chunk, LANES), BF16)
        return pl.pallas_call(
            kernel,
            out_shape=(jax.ShapeDtypeStruct((rows, cols, depth), BF16), part, part),
            in_specs=[pl.BlockSpec(memory_space=pltpu.SMEM)]
            + [pl.BlockSpec(memory_space=pltpu.VMEM)] * 9,
            out_specs=tuple([pl.BlockSpec(memory_space=pltpu.VMEM)] * 3),
            scratch_shapes=scratch,
            compiler_params=pltpu.CompilerParams(vmem_limit_bytes=VMEM_MAIN),
            name="block_grads",
        )(limit, tok, cot, below, right, corner, w_qkv, w_proj, logits, gain)

    return call


def finish(ours, theirs, logits, limit, depth, heads):
    core_rows = ours.shape[0]
    groups = depth // LANES
    half_q = 3 * depth // 2
    half_p = depth // 2
    body = half_q + half_p
    small_at = groups * body
    span = 2 * WIN - 1

    def kernel(limit, ours, theirs, logits, d_wq, d_wp, d_table, d_scale, d_gain, whole):
        core = lax.axis_index("hc")
        whole[pl.ds(pl.multiple_of(core * core_rows, 8), core_rows), :] = ours[...].astype(F32)
        other = pl.multiple_of((1 - core) * core_rows, 8)
        whole[pl.ds(other, core_rows), :] = theirs[...].astype(F32)
        for j in range(groups):
            tile = slice(j * LANES, (j + 1) * LANES)
            d_wq[:, tile] = whole[j * body : j * body + half_q, :]
            d_wp[:, tile] = whole[j * body + half_q : (j + 1) * body, :]
        small = whole[small_at : small_at + 32, :]
        near_map, far_map = table_maps(span, 2 * LANES)
        table = dot_nt(small[:16].astype(BF16), near_map)
        table = table + dot_nt(small[heads : heads + 16].astype(BF16), far_map)
        table = table[:heads, : span * span]
        sigma = jax.nn.sigmoid(logits[...])
        d_table[...] = table * (BIAS_RANGE * sigma * (1.0 - sigma))
        gains = [small[2 * heads + j : 2 * heads + j + 1, :] for j in range(groups)]
        d_gain[...] = jnp.concatenate(gains, axis=1).reshape(depth)
        lane = iota((1, LANES), 1)
        kept = jnp.zeros((1, LANES), F32)
        for h in range(heads):
            kept = jnp.where(lane == h, jnp.where(limit[h] < SCALE_CAP, 1.0, 0.0), kept)
        row = small[2 * heads + groups : 2 * heads + groups + 1, :] * kept
        d_scale[...] = row[:, :heads].reshape(heads)

    vmem = pl.BlockSpec(memory_space=pltpu.VMEM)
    return pl.pallas_call(
        kernel,
        out_shape=(
            jax.ShapeDtypeStruct((half_q, depth), F32),
            jax.ShapeDtypeStruct((half_p, depth), F32),
            jax.ShapeDtypeStruct(logits.shape, F32),
            jax.ShapeDtypeStruct((heads,), F32),
            jax.ShapeDtypeStruct((depth,), F32),
        ),
        in_specs=[pl.BlockSpec(memory_space=pltpu.SMEM), vmem, vmem, vmem],
        out_specs=(vmem,) * 5,
        scratch_shapes=[pltpu.VMEM((2 * core_rows, LANES), F32)],
        compiler_params=pltpu.CompilerParams(vmem_limit_bytes=VMEM_LAST),
        name="finish",
    )(limit, ours, theirs, logits)


def route(axes, move):
    sizes = [lax.axis_size(a) for a in axes]
    pairs = []
    for flat in range(math.prod(sizes)):
        left, where = flat, []
        for size in reversed(sizes):
            where.append(left % size)
            left //= size
        where = move(where[::-1], sizes)
        target = 0
        for place, size in zip(where, sizes):
            target = target * size + place
        pairs.append((flat, target))
    return pairs


GRID = ("hz", "hc", "wa")


def step(rows, cols):
    def move(where, sizes):
        high = (where[0] * sizes[1] + where[1] + rows) % (sizes[0] * sizes[1])
        return [high // sizes[1], high % sizes[1], (where[2] + cols) % sizes[2]]

    return move


FACE = ("hc", "wa", "ba")


def over(turn, by, crossed):
    def move(where, sizes):
        axis = 2 - (turn + (where[0] if crossed else 0)) % 2
        where = list(where)
        where[axis] = (where[axis] + by) % sizes[axis]
        return where

    return move


def along(by):
    return lambda where, sizes: [(where[0] + by) % sizes[0]]


def hand_out(blocks, place, axes, move):
    count = blocks.shape[0]
    total = lax.dynamic_index_in_dim(blocks, place, 0, keepdims=False).astype(F32)
    for by in range(count - 1, 0, -1):
        sent = lax.dynamic_index_in_dim(blocks, (place + by) % count, 0, keepdims=False)
        total = total + lax.ppermute(sent, axes, route(axes, move(by))).astype(F32)
    return total.astype(BF16)


def shards(tokens, cotangent, w_qkv, w_proj, table_logits, logit_scale, gain):
    images, rows, cols, depth = tokens.shape
    heads = logit_scale.shape[0]
    edge = WIN // 2
    both = jnp.concatenate([tokens, cotangent], 0)
    below = lax.ppermute(both[:, :edge], GRID, route(GRID, step(-1, 0)))
    left = both[:, :, :edge].reshape(2, rows * edge, depth)
    right = lax.ppermute(left, GRID, route(GRID, step(0, -1)))
    tip = left[:, : edge * edge]
    corner = lax.ppermute(tip, GRID, route(GRID, step(-1, -1)))

    cores, tall, across = lax.axis_size("hc"), lax.axis_size("hz"), lax.axis_size("wa")
    images_over = lax.axis_size("ba")
    owners = cores * tall * across
    used = 2 * depth // LANES * depth + 2 * heads + depth // LANES + 1
    unit = 8 * owners
    sent = -(-used // unit) * unit
    crossed = images_over == across
    order = (images_over, across, crossed)
    call = make_kernel(rows, cols, depth, heads, sent, across, order)
    d_moved, mine, given = call(
        logit_scale, tokens, cotangent, below, right, corner, w_qkv, w_proj, table_logits, gain
    )

    right = lax.ppermute(d_moved[: rows - edge, cols - edge :], GRID, route(GRID, step(0, 1)))
    lower = lax.ppermute(d_moved[rows - edge :, : cols - edge], GRID, route(GRID, step(1, 0)))
    cross = lax.ppermute(
        d_moved[rows - edge :, cols - edge :], GRID, route(GRID, step(1, 1))
    )
    upper = jnp.concatenate([cross, lower], 1)
    main = jnp.concatenate([right, d_moved[: rows - edge, : cols - edge]], 1)
    back = jnp.concatenate([upper, main], 0)[None]
    d_tokens = (cotangent.astype(F32) + back.astype(F32)).astype(BF16)

    swap = route(("hc",), lambda where, sizes: [1 - where[0]])
    taken = lax.ppermute(given, "hc", swap)
    summed = (mine.astype(F32) + taken.astype(F32)).astype(BF16)
    piece = sent // owners
    core, column, image = lax.axis_index("hc"), lax.axis_index("wa"), lax.axis_index("ba")
    turn = core if crossed else 0
    moves = (lambda by: over(0, by, crossed)), (lambda by: over(1, by, crossed))
    summed = hand_out(summed, image + (column - image) * turn, FACE, moves[0])
    summed = hand_out(summed, column + (image - column) * turn, FACE, moves[1])
    summed = summed.reshape(tall, piece, LANES)
    total = hand_out(summed, lax.axis_index("hz"), ("hz",), along)
    spread = jnp.broadcast_to(total[None], (tall * across, piece, LANES))
    ours = lax.all_to_all(spread, ("wa", "hz"), 0, 0, tiled=True)
    ours = ours.reshape(sent // cores, LANES)
    theirs = lax.ppermute(ours, "hc", swap)
    d_wq, d_wp, d_table, d_scale, d_gain = finish(
        ours, theirs, table_logits, logit_scale, depth, heads
    )
    return (d_tokens, d_wq.T, d_wp.T, d_table, d_scale, d_gain)


def solution(mesh):
    sizes = mesh.shape
    devices = mesh.devices.reshape(sizes["ha"] // 2, 2, sizes["wa"], sizes["ba"])
    inner = Mesh(devices, ("hz", "hc", "wa", "ba"))
    image = P("ba", ("hz", "hc"), "wa", None)
    return jax.shard_map(
        shards,
        mesh=inner,
        in_specs=(image, image, P(), P(), P(), P(), P()),
        out_specs=(image, P(None, "ba"), P(None, "ba"), P(), P(), P()),
        check_vma=False,
    )
```

```python
import functools
import math

import jax
import jax.numpy as jnp
from jax import lax
from jax.experimental import pallas as pl
from jax.experimental.pallas import tpu as pltpu
from jax.sharding import Mesh
from jax.sharding import PartitionSpec as P

WIN = 8
TOKENS = WIN * WIN
LANES = 128
EPS_NORM = 1e-05
MASK_FILL = -100.0
SCALE_CAP = math.log(100.0)
BIAS_RANGE = 16.0
LOG2_E = math.log2(math.e)
VMEM_MAIN = 36 << 20
VMEM_LAST = 12 << 20
F32 = jnp.float32
BF16 = jnp.bfloat16


def dot_nn(left, right):
    return lax.dot_general(left, right, (((1,), (0,)), ((), ())), preferred_element_type=F32)


def dot_nt(left, right):
    return lax.dot_general(left, right, (((1,), (1,)), ((), ())), preferred_element_type=F32)


def dot_tn(left, right):
    return lax.dot_general(left, right, (((0,), (0,)), ((), ())), preferred_element_type=F32)


def iota(shape, dim):
    return lax.broadcasted_iota(jnp.int32, shape, dim)


def split(value):
    high = value.astype(BF16)
    return high, (value - high.astype(F32)).astype(BF16)


def group_sum(value, ones, fine=True):
    high, low = split(value)
    width = ones.shape[0]
    parts = []
    for start in range(0, value.shape[1], width):
        part = slice(start, start + width)
        total = dot_nn(high[:, part], ones)
        parts.append(total + dot_nn(low[:, part], ones) if fine else total)
    return jnp.concatenate(parts, axis=1)


def table_maps(span, used):
    entry = iota((used, LANES), 0)
    lane = iota((used, LANES), 1)
    same_row = entry // span == lane // WIN
    near = jnp.logical_and(same_row, entry % span == lane % WIN)
    far = jnp.logical_and(same_row, entry % span == lane % WIN + WIN)
    return near.astype(F32).astype(BF16), far.astype(F32).astype(BF16)


def repeat(count, step, carry=0):
    for p in range(count):
        carry = step(p, carry)
    return carry


def pipeline(items, stages):
    for start in range(len(items) + len(stages) - 1):
        for back, stage in enumerate(stages):
            if 0 <= start - back < len(items):
                stage(*items[start - back])


def make_kernel(rows, cols, depth, heads, sent_rows, across, order):
    head_dim = depth // heads
    per_tile = LANES // head_dim
    groups = heads // per_tile
    col_windows = cols // WIN
    row_windows = rows // WIN
    pairs = row_windows * col_windows // 2
    pairs_across = col_windows // 2
    stacked = per_tile * TOKENS
    pair = 2 * TOKENS
    tokens = rows * cols
    span = 2 * WIN - 1
    half_q = 3 * depth // 2
    half_p = depth // 2
    body = half_q + half_p
    small_at = groups * body
    small_rows = sent_rows - small_at
    core_rows = sent_rows // 2
    edge = WIN // 2
    pitch = cols + WIN
    outer, inner, crossed = order
    chunk = core_rows // across

    def kernel(
        limit,
        tok,
        cot,
        below,
        right,
        corner,
        w_qkv,
        w_proj,
        logits,
        gain,
        d_img,
        mine,
        given,
        xb,
        uf,
        unit_s,
        inv,
        q_low,
        q_turn,
        k_hi,
        k_lo,
        val,
        prob,
        prob_low,
        raw,
        d_prob,
        d_low,
        att,
        d_prj,
        d_att,
        d_qkv,
        d_unit,
        bias,
        d_bias,
        d_sc,
        small,
        sums,
        padded,
        wide_x,
        wide_u,
    ):
        core = lax.axis_index("hc")
        down = lax.axis_index("hz") * lax.axis_size("hc") + core
        last_row = (down == lax.axis_size("hz") * lax.axis_size("hc") - 1).astype(jnp.int32)
        last_col = (lax.axis_index("wa") == lax.axis_size("wa") - 1).astype(jnp.int32)
        half = iota((1, LANES), 1) < TOKENS
        wide = 2 * LANES
        ones = (iota((wide, wide), 0) // head_dim == iota((wide, wide), 1) // head_dim).astype(F32)
        ones = ones.astype(BF16)
        owner = iota((1, wide), 1) % LANES // head_dim
        head_low = [(owner == h).astype(F32).astype(BF16) for h in range(per_tile)]
        top_rows = (iota((pair, LANES), 0) < TOKENS).astype(F32)
        top_rows, low_rows = top_rows.astype(BF16), (1.0 - top_rows).astype(BF16)
        left_lanes = half.astype(F32)
        left_lanes, right_lanes = left_lanes.astype(BF16), (1.0 - left_lanes).astype(BF16)
        by_head = iota((1, depth), 1) // head_dim
        scale = jnp.zeros((1, depth), F32)
        for h in range(heads):
            scale = jnp.where(by_head == h, limit[h], scale)
        scale = jnp.exp(jnp.minimum(scale, SCALE_CAP))

        for which, (own, wide_of) in enumerate(((tok, wide_x), (cot, wide_u))):
            edges = right[which].astype(F32)
            ends = corner[which].astype(F32)
            for i in range(rows):
                if i + edge < rows:
                    row = own[0, i + edge].astype(F32)
                    side = edges[i * edge : (i + 1) * edge]
                else:
                    row = below[which, i + edge - rows].astype(F32)
                    side = ends[(i + edge - rows) * edge : (i + edge - rows + 1) * edge]
                at = i * pitch
                for j in range(groups):
                    tile = slice(j * LANES, (j + 1) * LANES)
                    wide_of[j, at : at + cols, :] = row[:, tile]
                    wide_of[j, at + cols : at + cols + edge, :] = side[:, tile]

        def window_rows(wide_of, p):
            tiles = []
            for j in range(groups):
                pieces = []
                for w in range(2):
                    i0 = p // pairs_across * WIN
                    j0 = (p % pairs_across * 2 + w) * WIN + edge
                    for r in range(WIN):
                        at = (i0 + r) * pitch + j0
                        pieces.append(wide_of[j, at : at + WIN, :])
                tiles.append(jnp.concatenate(pieces, axis=0))
            return jnp.concatenate(tiles, axis=1)

        def project(p, carry):
            place = pl.ds(p * pair, pair)
            x = window_rows(wide_x, p).astype(BF16)
            uf[place, :] = window_rows(wide_u, p)
            xb[place, :] = x
            qkv = dot_nn(x, w_qkv[...]).astype(BF16)
            val[place, :] = qkv[:, 2 * depth :]
            both = qkv[:, : 2 * depth].astype(F32)
            root = lax.rsqrt(group_sum(both * both, ones) + 1.0)
            unit = both * root
            unit_s[place, :] = unit
            inv[place, :] = root[:, depth:]
            q_low[place, :] = qkv[:, :depth]
            q_turn[p] = (root[:, :depth] * scale).T
            k_hi[place, :], k_lo[place, :] = split(unit[:, depth:])
            return carry

        repeat(pairs, project)

        sub = iota((WIN, LANES), 0)
        lane = iota((WIN, LANES), 1)
        near_map, far_map = table_maps(span, 2 * LANES)
        padded[...] = jnp.zeros_like(padded)
        padded[:heads, : span * span] = jax.nn.sigmoid(logits[...]) * (BIAS_RANGE * LOG2_E)
        table = padded[...]
        first = table.astype(BF16)
        second, third = split(table - first.astype(F32))
        table_a = dot_nn(first, near_map) + (dot_nn(second, near_map) + dot_nn(third, near_map))
        table_b = dot_nn(first, far_map) + (dot_nn(second, far_map) + dot_nn(third, far_map))
        for h in range(heads):
            near = jnp.broadcast_to(table_a[h : h + 1, :], (WIN, LANES))
            far = jnp.broadcast_to(table_b[h : h + 1, :], (WIN, LANES))
            near = pltpu.roll(near, LANES - WIN + 1, 1, stride=1, stride_axis=0)
            far = pltpu.roll(far, 1, 1, stride=1, stride_axis=0)
            line = jnp.where(lane % WIN <= sub, near, far)
            for r in range(WIN):
                one = pltpu.roll(line, (LANES - (WIN - 1 - r) * WIN) % LANES, 1)
                two = pltpu.roll(line, (LANES + TOKENS - (WIN - 1 - r) * WIN) % LANES, 1)
                at = h * TOKENS + r * WIN
                bias[at : at + WIN, :] = jnp.where(half, one, two)

        key = iota((TOKENS, LANES), 0)
        query = iota((TOKENS, LANES), 1) % TOKENS
        split_r = ((key // WIN) >= edge) != ((query // WIN) >= edge)
        split_c = ((key % WIN) >= edge) != ((query % WIN) >= edge)
        split_c = jnp.logical_and(split_c, iota((TOKENS, LANES), 1) >= TOKENS)
        mask_r = jnp.where(split_r, MASK_FILL * LOG2_E, 0.0)
        mask_c = jnp.where(split_c, MASK_FILL * LOG2_E, 0.0)

        def beside(ref, at, tile):
            one = ref[pl.ds(at, TOKENS), tile]
            two = ref[pl.ds(at + TOKENS, TOKENS), tile]
            return jnp.concatenate([one, two], axis=1)

        def stack(block):
            return jnp.concatenate([block * head_low[h] for h in range(per_tile)], axis=0)

        def diagonal(ref, at, tile):
            block = ref[pl.ds(at, pair), tile]
            return jnp.concatenate([block * top_rows, block * low_rows], axis=1)

        def turned(ref, at, tile):
            block = ref[pl.ds(at, pair), tile].T
            return jnp.concatenate([block * left_lanes, block * right_lanes], axis=0)

        def gather_heads(out):
            total = out[:TOKENS]
            for h in range(1, per_tile):
                total = jnp.where(owner == h, out[h * TOKENS : (h + 1) * TOKENS], total)
            return total

        tiles = [(p, g) for p in range(pairs) for g in range(groups)]

        def lanes_of(g):
            return slice(g * LANES, (g + 1) * LANES)

        def score(p, g):
            keys = stack(beside(k_hi, p * pair, lanes_of(g)))
            keys_low = stack(beside(k_lo, p * pair, lanes_of(g)))
            queries = turned(q_low, p * pair, lanes_of(g))
            raw[p, g] = dot_nn(keys, queries) + dot_nn(keys_low, queries)

        def soften(p, g):
            masks = []
            if p // pairs_across == row_windows - 1:
                masks.append(mask_r * last_row.astype(F32))
            if p % pairs_across == pairs_across - 1:
                masks.append(mask_c * last_col.astype(F32))
            for h in range(per_tile):
                place = slice(h * TOKENS, (h + 1) * TOKENS)
                head = g * per_tile + h
                line = q_turn[p, head * head_dim : head * head_dim + 1, :] * LOG2_E
                added = bias[head * TOKENS : (head + 1) * TOKENS, :]
                if masks:
                    added = added + functools.reduce(jnp.minimum, masks)
                s = raw[p, g, place, :] * line + added
                e = jnp.exp2(s - jnp.max(s, axis=0, keepdims=True))
                pr = e * (1.0 / jnp.sum(e, axis=0, keepdims=True))
                prob[p, g, place, :] = pr
                prob_low[p, g, place, :] = pr.astype(BF16)

        def attend(p, g):
            at, tile = p * pair, lanes_of(g)
            out = dot_tn(prob_low[p, g], stack(beside(val, at, tile)))
            att[at : at + TOKENS, tile] = out[:TOKENS, :LANES].astype(BF16)
            att[at + TOKENS : at + pair, tile] = out[TOKENS:, LANES:].astype(BF16)

        pipeline(tiles, (score, soften, attend))

        gains = gain[...].reshape(1, depth)

        def norm(p, d_gain):
            place = pl.ds(p * pair, pair)
            proj = dot_nn(att[place, :], w_proj[...])
            centre = proj - jnp.mean(proj, -1, keepdims=True)
            std = lax.rsqrt(jnp.mean(centre * centre, -1, keepdims=True) + EPS_NORM)
            normed = centre * std
            up = uf[place, :]
            d_gain = d_gain + jnp.sum(up * normed, axis=0, keepdims=True)
            u = up * gains
            d_p = std * (
                u - jnp.mean(u, -1, keepdims=True) - normed * jnp.mean(u * normed, -1, keepdims=True)
            )
            d_p = d_p.astype(BF16)
            d_prj[place, :] = d_p
            return d_gain

        d_gain = repeat(pairs, norm, jnp.zeros((1, depth), F32))

        w_proj_turned = w_proj[...].T

        def spread(p, carry):
            place = pl.ds(p * pair, pair)
            d_att[place, :] = dot_nn(d_prj[place, :], w_proj_turned).astype(BF16)
            return carry

        repeat(pairs, spread)

        def rise(p, g):
            values = stack(beside(val, p * pair, lanes_of(g)))
            d_prob[p, g] = dot_nn(values, turned(d_att, p * pair, lanes_of(g)))

        def harden(p, g):
            for h in range(per_tile):
                place = slice(h * TOKENS, (h + 1) * TOKENS)
                head = g * per_tile + h
                of = slice(head * TOKENS, (head + 1) * TOKENS)
                pr = prob[p, g, place, :]
                pd = pr * d_prob[p, g, place, :]
                d_s = pd - pr * jnp.sum(pd, axis=0, keepdims=True)
                if p == 0:
                    d_bias[of, :] = d_s
                else:
                    d_bias[of, :] += d_s
                d_s = d_s * q_turn[p, head * head_dim : head * head_dim + 1, :]
                by_scale = (d_s * raw[p, g, place, :]).reshape(WIN, WIN, LANES)
                of = slice(head * WIN, (head + 1) * WIN)
                if p == 0:
                    d_sc[of, :] = jnp.sum(by_scale, axis=0)
                else:
                    d_sc[of, :] += jnp.sum(by_scale, axis=0)
                d_low[p, g, place, :] = d_s.astype(BF16)

        def fall(p, g):
            at, tile = p * pair, lanes_of(g)
            key_tile = slice(depth + g * LANES, depth + (g + 1) * LANES)
            val_tile = slice(2 * depth + g * LANES, 2 * depth + (g + 1) * LANES)
            d_v = gather_heads(dot_nn(prob_low[p, g], diagonal(d_att, at, tile))).astype(BF16)
            d_qkv[at : at + TOKENS, val_tile] = d_v[:, :LANES]
            d_qkv[at + TOKENS : at + pair, val_tile] = d_v[:, LANES:]
            d_k = gather_heads(dot_nn(d_low[p, g], diagonal(q_low, at, tile)))
            d_unit[at : at + TOKENS, key_tile] = d_k[:, :LANES]
            d_unit[at + TOKENS : at + pair, key_tile] = d_k[:, LANES:]
            d_q = dot_tn(d_low[p, g], stack(beside(k_hi, at, tile)))
            d_unit[at : at + TOKENS, tile] = d_q[:TOKENS, :LANES]
            d_unit[at + TOKENS : at + pair, tile] = d_q[TOKENS:, LANES:]

        pipeline(tiles, (rise, harden, fall))

        w_qkv_turned = w_qkv[...].T

        def flatten(p, carry):
            place = pl.ds(p * pair, pair)
            unit = unit_s[place, :]
            d_u = d_unit[place, :]
            d_u = d_u - unit * group_sum(unit * d_u, ones, False)
            d_qkv[place, :depth] = d_u[:, :depth].astype(BF16)
            d_qkv[place, depth : 2 * depth] = (inv[place, :] * d_u[:, depth:]).astype(BF16)
            flat = dot_nn(d_qkv[place, :], w_qkv_turned)
            for w in range(2):
                i0 = p // pairs_across * WIN
                j0 = (p % pairs_across * 2 + w) * WIN
                for r in range(WIN):
                    piece = flat[w * TOKENS + r * WIN : w * TOKENS + (r + 1) * WIN]
                    d_img[i0 + r, pl.ds(j0, WIN), :] = piece.astype(BF16)
            return carry

        repeat(pairs, flatten)

        d_wp = dot_tn(d_prj[...], att[...])
        d_wq = dot_tn(d_qkv[...], xb[...])
        for b in range(2):
            for j in range(groups):
                tile = slice(j * LANES, (j + 1) * LANES)
                at = b * sent_rows + j * body
                sums[at : at + half_q, :] = d_wq[b * half_q : (b + 1) * half_q, tile].astype(BF16)
                at = at + half_q
                sums[at : at + half_p, :] = d_wp[b * half_p : (b + 1) * half_p, tile].astype(BF16)

        small[...] = jnp.zeros_like(small)
        for h in range(heads):
            line = jnp.zeros((WIN, LANES), F32)
            for r in range(WIN):
                at = h * TOKENS + r * WIN
                part = d_bias[at : at + WIN, :]
                part = jnp.where(half, part + pltpu.roll(part, TOKENS, 1), 0.0)
                line = line + pltpu.roll(part, (WIN - 1 - r) * WIN, 1)
            near, far = jnp.zeros_like(line), jnp.zeros_like(line)
            for c in range(WIN):
                own = jnp.where(sub == c, line, 0.0)
                near = near + pltpu.roll(own, WIN - 1 - c, 1)
                far = far + pltpu.roll(own, LANES - 1 - c, 1)
            near = jnp.where(lane % WIN >= WIN - 1 - sub, near, 0.0)
            far = jnp.where(lane % WIN + sub + 1 <= WIN - 1, far, 0.0)
            small[h : h + 1, :] = jnp.sum(near, axis=0, keepdims=True)
            small[heads + h : heads + h + 1, :] = jnp.sum(far, axis=0, keepdims=True)
        for j in range(groups):
            small[2 * heads + j : 2 * heads + j + 1, :] = d_gain[:, j * LANES : (j + 1) * LANES]
        line = jnp.zeros((1, LANES), F32)
        for h in range(heads):
            total = jnp.sum(d_sc[h * WIN : (h + 1) * WIN, :], axis=0, keepdims=True)
            total = jnp.sum(total, axis=1, keepdims=True)
            line = line + jnp.where(iota((1, LANES), 1) == h, total, 0.0)
        at = 2 * heads + groups
        small[at : at + 1, :] = line
        for b in range(2):
            at = b * sent_rows + small_at
            sums[at : at + small_rows, :] = small[...].astype(BF16)
        for out, whose in ((mine, core), (given, 1 - core)):
            turn = whose if crossed else 0
            for f in range(outer):
                for n in range(inner):
                    image = f + (n - f) * turn
                    column = n + (f - n) * turn
                    at = image * sent_rows + whose * core_rows + column * chunk
                    out[f, n] = sums[pl.ds(pl.multiple_of(at, 8), chunk), :]

    def call(limit, tok, cot, below, right, corner, w_qkv, w_proj, logits, gain):
        vmem = pltpu.VMEM
        scratch = [
            vmem((tokens, depth), BF16),
            vmem((tokens, depth), F32),
            vmem((tokens, 2 * depth), F32),
            vmem((tokens, depth), F32),
            vmem((tokens, depth), BF16),
            vmem((pairs, depth, pair), F32),
            vmem((tokens, depth), BF16),
            vmem((tokens, depth), BF16),
            vmem((tokens, depth), BF16),
            vmem((pairs, groups, stacked, LANES), F32),
            vmem((pairs, groups, stacked, LANES), BF16),
            vmem((pairs, groups, stacked, LANES), F32),
            vmem((pairs, groups, stacked, LANES), F32),
            vmem((pairs, groups, stacked, LANES), BF16),
            vmem((tokens, depth), BF16),
            vmem((tokens, depth), BF16),
            vmem((tokens, depth), BF16),
            vmem((tokens, 3 * depth), BF16),
            vmem((tokens, 2 * depth), F32),
            vmem((heads * TOKENS, LANES), F32),
            vmem((heads * TOKENS, LANES), F32),
            vmem((heads * WIN, LANES), F32),
            vmem((small_rows, LANES), F32),
            vmem((2 * sent_rows, LANES), BF16),
            vmem((16, 2 * LANES), F32),
            vmem((groups, rows * pitch, LANES), F32),
            vmem((groups, rows * pitch, LANES), F32),
        ]
        part = jax.ShapeDtypeStruct((outer, inner, chunk, LANES), BF16)
        return pl.pallas_call(
            kernel,
            out_shape=(jax.ShapeDtypeStruct((rows, cols, depth), BF16), part, part),
            in_specs=[pl.BlockSpec(memory_space=pltpu.SMEM)]
            + [pl.BlockSpec(memory_space=pltpu.VMEM)] * 9,
            out_specs=tuple([pl.BlockSpec(memory_space=pltpu.VMEM)] * 3),
            scratch_shapes=scratch,
            compiler_params=pltpu.CompilerParams(vmem_limit_bytes=VMEM_MAIN),
            name="block_grads",
        )(limit, tok, cot, below, right, corner, w_qkv, w_proj, logits, gain)

    return call


def finish(ours, theirs, logits, limit, depth, heads):
    core_rows = ours.shape[0]
    groups = depth // LANES
    half_q = 3 * depth // 2
    half_p = depth // 2
    body = half_q + half_p
    small_at = groups * body
    span = 2 * WIN - 1

    def kernel(limit, ours, theirs, logits, d_wq, d_wp, d_table, d_scale, d_gain, whole):
        core = lax.axis_index("hc")
        whole[pl.ds(pl.multiple_of(core * core_rows, 8), core_rows), :] = ours[...].astype(F32)
        other = pl.multiple_of((1 - core) * core_rows, 8)
        whole[pl.ds(other, core_rows), :] = theirs[...].astype(F32)
        for j in range(groups):
            tile = slice(j * LANES, (j + 1) * LANES)
            d_wq[:, tile] = whole[j * body : j * body + half_q, :]
            d_wp[:, tile] = whole[j * body + half_q : (j + 1) * body, :]
        small = whole[small_at : small_at + 32, :]
        near_map, far_map = table_maps(span, 2 * LANES)
        table = dot_nt(small[:16].astype(BF16), near_map)
        table = table + dot_nt(small[heads : heads + 16].astype(BF16), far_map)
        table = table[:heads, : span * span]
        sigma = jax.nn.sigmoid(logits[...])
        d_table[...] = table * (BIAS_RANGE * sigma * (1.0 - sigma))
        gains = [small[2 * heads + j : 2 * heads + j + 1, :] for j in range(groups)]
        d_gain[...] = jnp.concatenate(gains, axis=1).reshape(depth)
        lane = iota((1, LANES), 1)
        kept = jnp.zeros((1, LANES), F32)
        for h in range(heads):
            kept = jnp.where(lane == h, jnp.where(limit[h] < SCALE_CAP, 1.0, 0.0), kept)
        row = small[2 * heads + groups : 2 * heads + groups + 1, :] * kept
        d_scale[...] = row[:, :heads].reshape(heads)

    vmem = pl.BlockSpec(memory_space=pltpu.VMEM)
    return pl.pallas_call(
        kernel,
        out_shape=(
            jax.ShapeDtypeStruct((half_q, depth), F32),
            jax.ShapeDtypeStruct((half_p, depth), F32),
            jax.ShapeDtypeStruct(logits.shape, F32),
            jax.ShapeDtypeStruct((heads,), F32),
            jax.ShapeDtypeStruct((depth,), F32),
        ),
        in_specs=[pl.BlockSpec(memory_space=pltpu.SMEM), vmem, vmem, vmem],
        out_specs=(vmem,) * 5,
        scratch_shapes=[pltpu.VMEM((2 * core_rows, LANES), F32)],
        compiler_params=pltpu.CompilerParams(vmem_limit_bytes=VMEM_LAST),
        name="finish",
    )(limit, ours, theirs, logits)


def route(axes, move):
    sizes = [lax.axis_size(a) for a in axes]
    pairs = []
    for flat in range(math.prod(sizes)):
        left, where = flat, []
        for size in reversed(sizes):
            where.append(left % size)
            left //= size
        where = move(where[::-1], sizes)
        target = 0
        for place, size in zip(where, sizes):
            target = target * size + place
        pairs.append((flat, target))
    return pairs


GRID = ("hz", "hc", "wa")


def step(rows, cols):
    def move(where, sizes):
        high = (where[0] * sizes[1] + where[1] + rows) % (sizes[0] * sizes[1])
        return [high // sizes[1], high % sizes[1], (where[2] + cols) % sizes[2]]

    return move


FACE = ("hc", "wa", "ba")


def over(turn, by, crossed):
    def move(where, sizes):
        axis = 2 - (turn + (where[0] if crossed else 0)) % 2
        where = list(where)
        where[axis] = (where[axis] + by) % sizes[axis]
        return where

    return move


def along(by):
    return lambda where, sizes: [(where[0] + by) % sizes[0]]


def hand_out(blocks, place, axes, move):
    count = blocks.shape[0]
    total = lax.dynamic_index_in_dim(blocks, place, 0, keepdims=False).astype(F32)
    for by in range(count - 1, 0, -1):
        sent = lax.dynamic_index_in_dim(blocks, (place + by) % count, 0, keepdims=False)
        total = total + lax.ppermute(sent, axes, route(axes, move(by))).astype(F32)
    return total.astype(BF16)


def shards(tokens, cotangent, w_qkv, w_proj, table_logits, logit_scale, gain):
    images, rows, cols, depth = tokens.shape
    heads = logit_scale.shape[0]
    edge = WIN // 2
    both = jnp.concatenate([tokens, cotangent], 0)
    top = both[:, :edge]
    left = both[:, edge:, :edge].reshape(2, (rows - edge) * edge, depth)
    tip = both[:, :edge, :edge].reshape(2, edge * edge, depth)
    below = lax.ppermute(top, GRID, route(GRID, step(-1, 0)))
    right = lax.ppermute(left, GRID, route(GRID, step(0, -1)))
    corner = lax.ppermute(tip, GRID, route(GRID, step(-1, -1)))

    cores, tall, across = lax.axis_size("hc"), lax.axis_size("hz"), lax.axis_size("wa")
    images_over = lax.axis_size("ba")
    owners = cores * tall * across
    used = 2 * depth // LANES * depth + 2 * heads + depth // LANES + 1
    unit = 8 * owners
    sent = -(-used // unit) * unit
    crossed = images_over == across
    order = (images_over, across, crossed)
    call = make_kernel(rows, cols, depth, heads, sent, across, order)
    d_moved, mine, given = call(
        logit_scale, tokens, cotangent, below, right, corner, w_qkv, w_proj, table_logits, gain
    )

    right = lax.ppermute(d_moved[: rows - edge, cols - edge :], GRID, route(GRID, step(0, 1)))
    lower = lax.ppermute(d_moved[rows - edge :, : cols - edge], GRID, route(GRID, step(1, 0)))
    cross = lax.ppermute(
        d_moved[rows - edge :, cols - edge :], GRID, route(GRID, step(1, 1))
    )
    upper = jnp.concatenate([cross, lower], 1)
    main = jnp.concatenate([right, d_moved[: rows - edge, : cols - edge]], 1)
    back = jnp.concatenate([upper, main], 0)[None]
    d_tokens = (cotangent.astype(F32) + back.astype(F32)).astype(BF16)

    swap = route(("hc",), lambda where, sizes: [1 - where[0]])
    one = jnp.where(lax.axis_index("hc") < 0, 0.0, 1.0).astype(BF16)
    taken = lax.ppermute(given * one, "hc", swap)
    summed = (mine.astype(F32) + taken.astype(F32)).astype(BF16)
    piece = sent // owners
    core, column, image = lax.axis_index("hc"), lax.axis_index("wa"), lax.axis_index("ba")
    turn = core if crossed else 0
    moves = (lambda by: over(0, by, crossed)), (lambda by: over(1, by, crossed))
    summed = hand_out(summed, image + (column - image) * turn, FACE, moves[0])
    summed = hand_out(summed, column + (image - column) * turn, FACE, moves[1])
    summed = summed.reshape(tall, piece, LANES)
    total = hand_out(summed, lax.axis_index("hz"), ("hz",), along)
    spread = jnp.broadcast_to(total[None], (tall * across, piece, LANES))
    ours = lax.all_to_all(spread, ("wa", "hz"), 0, 0, tiled=True)
    ours = ours.reshape(sent // cores, LANES)
    theirs = lax.ppermute(ours, "hc", swap)
    d_wq, d_wp, d_table, d_scale, d_gain = finish(
        ours, theirs, table_logits, logit_scale, depth, heads
    )
    return (d_tokens, d_wq.T, d_wp.T, d_table, d_scale, d_gain)


def solution(mesh):
    sizes = mesh.shape
    devices = mesh.devices.reshape(sizes["ha"] // 2, 2, sizes["wa"], sizes["ba"])
    inner = Mesh(devices, ("hz", "hc", "wa", "ba"))
    image = P("ba", ("hz", "hc"), "wa", None)
    return jax.shard_map(
        shards,
        mesh=inner,
        in_specs=(image, image, P(), P(), P(), P(), P()),
        out_specs=(image, P(None, "ba"), P(None, "ba"), P(), P(), P()),
        check_vma=False,
    )
```

```python
import functools
import math

import jax
import jax.numpy as jnp
from jax import lax
from jax.experimental import pallas as pl
from jax.experimental.pallas import tpu as pltpu
from jax.sharding import Mesh
from jax.sharding import PartitionSpec as P

WIN = 8
TOKENS = WIN * WIN
LANES = 128
EPS_NORM = 1e-05
MASK_FILL = -100.0
SCALE_CAP = math.log(100.0)
BIAS_RANGE = 16.0
LOG2_E = math.log2(math.e)
VMEM_MAIN = 36 << 20
VMEM_LAST = 12 << 20
F32 = jnp.float32
BF16 = jnp.bfloat16


def dot_nn(left, right):
    return lax.dot_general(left, right, (((1,), (0,)), ((), ())), preferred_element_type=F32)


def dot_nt(left, right):
    return lax.dot_general(left, right, (((1,), (1,)), ((), ())), preferred_element_type=F32)


def dot_tn(left, right):
    return lax.dot_general(left, right, (((0,), (0,)), ((), ())), preferred_element_type=F32)


def iota(shape, dim):
    return lax.broadcasted_iota(jnp.int32, shape, dim)


def split(value):
    high = value.astype(BF16)
    return high, (value - high.astype(F32)).astype(BF16)


def group_sum(value, ones, fine=True):
    high, low = split(value)
    width = ones.shape[0]
    parts = []
    for start in range(0, value.shape[1], width):
        part = slice(start, start + width)
        total = dot_nn(high[:, part], ones)
        parts.append(total + dot_nn(low[:, part], ones) if fine else total)
    return jnp.concatenate(parts, axis=1)


def table_maps(span, used):
    entry = iota((used, LANES), 0)
    lane = iota((used, LANES), 1)
    same_row = entry // span == lane // WIN
    near = jnp.logical_and(same_row, entry % span == lane % WIN)
    far = jnp.logical_and(same_row, entry % span == lane % WIN + WIN)
    return near.astype(F32).astype(BF16), far.astype(F32).astype(BF16)


def repeat(count, step, carry=0):
    for p in range(count):
        carry = step(p, carry)
    return carry


def pipeline(items, stages):
    for start in range(len(items) + len(stages)):
        for back, stage in zip((0, 2, 3), stages):
            if 0 <= start - back < len(items):
                stage(*items[start - back])


def make_kernel(rows, cols, depth, heads, sent_rows, across, order):
    head_dim = depth // heads
    per_tile = LANES // head_dim
    groups = heads // per_tile
    col_windows = cols // WIN
    row_windows = rows // WIN
    pairs = row_windows * col_windows // 2
    pairs_across = col_windows // 2
    stacked = per_tile * TOKENS
    pair = 2 * TOKENS
    tokens = rows * cols
    span = 2 * WIN - 1
    half_q = 3 * depth // 2
    half_p = depth // 2
    body = half_q + half_p
    small_at = groups * body
    small_rows = sent_rows - small_at
    core_rows = sent_rows // 2
    edge = WIN // 2
    pitch = cols + WIN
    outer, inner, crossed = order
    chunk = core_rows // across

    def kernel(
        limit,
        tok,
        cot,
        below,
        right,
        corner,
        w_qkv,
        w_proj,
        logits,
        gain,
        d_img,
        mine,
        given,
        xb,
        uf,
        unit_s,
        inv,
        q_low,
        q_turn,
        k_hi,
        k_lo,
        val,
        prob,
        prob_low,
        raw,
        d_prob,
        d_low,
        att,
        d_prj,
        d_att,
        d_qkv,
        d_unit,
        bias,
        d_bias,
        d_sc,
        small,
        sums,
        padded,
        wide_x,
        wide_u,
    ):
        core = lax.axis_index("hc")
        down = lax.axis_index("hz") * lax.axis_size("hc") + core
        last_row = (down == lax.axis_size("hz") * lax.axis_size("hc") - 1).astype(jnp.int32)
        last_col = (lax.axis_index("wa") == lax.axis_size("wa") - 1).astype(jnp.int32)
        half = iota((1, LANES), 1) < TOKENS
        wide = 2 * LANES
        ones = (iota((wide, wide), 0) // head_dim == iota((wide, wide), 1) // head_dim).astype(F32)
        ones = ones.astype(BF16)
        owner = iota((1, wide), 1) % LANES // head_dim
        head_low = [(owner == h).astype(F32).astype(BF16) for h in range(per_tile)]
        top_rows = (iota((pair, LANES), 0) < TOKENS).astype(F32)
        top_rows, low_rows = top_rows.astype(BF16), (1.0 - top_rows).astype(BF16)
        left_lanes = half.astype(F32)
        left_lanes, right_lanes = left_lanes.astype(BF16), (1.0 - left_lanes).astype(BF16)
        by_head = iota((1, depth), 1) // head_dim
        scale = jnp.zeros((1, depth), F32)
        for h in range(heads):
            scale = jnp.where(by_head == h, limit[h], scale)
        scale = jnp.exp(jnp.minimum(scale, SCALE_CAP))

        for which, (own, wide_of) in enumerate(((tok, wide_x), (cot, wide_u))):
            edges = right[which].astype(F32)
            ends = corner[which].astype(F32)
            for i in range(rows):
                if i + edge < rows:
                    row = own[0, i + edge].astype(F32)
                    side = edges[i * edge : (i + 1) * edge]
                else:
                    row = below[which, i + edge - rows].astype(F32)
                    side = ends[(i + edge - rows) * edge : (i + edge - rows + 1) * edge]
                at = i * pitch
                for j in range(groups):
                    tile = slice(j * LANES, (j + 1) * LANES)
                    wide_of[j, at : at + cols, :] = row[:, tile]
                    wide_of[j, at + cols : at + cols + edge, :] = side[:, tile]

        def window_rows(wide_of, p):
            tiles = []
            for j in range(groups):
                pieces = []
                for w in range(2):
                    i0 = p // pairs_across * WIN
                    j0 = (p % pairs_across * 2 + w) * WIN + edge
                    for r in range(WIN):
                        at = (i0 + r) * pitch + j0
                        pieces.append(wide_of[j, at : at + WIN, :])
                tiles.append(jnp.concatenate(pieces, axis=0))
            return jnp.concatenate(tiles, axis=1)

        def project(p, carry):
            place = pl.ds(p * pair, pair)
            x = window_rows(wide_x, p).astype(BF16)
            uf[place, :] = window_rows(wide_u, p)
            xb[place, :] = x
            qkv = dot_nn(x, w_qkv[...]).astype(BF16)
            val[place, :] = qkv[:, 2 * depth :]
            both = qkv[:, : 2 * depth].astype(F32)
            root = lax.rsqrt(group_sum(both * both, ones) + 1.0)
            unit = both * root
            unit_s[place, :] = unit
            inv[place, :] = root[:, depth:]
            q_low[place, :] = qkv[:, :depth]
            q_turn[p] = (root[:, :depth] * scale).T
            k_hi[place, :], k_lo[place, :] = split(unit[:, depth:])
            return carry

        repeat(pairs, project)

        sub = iota((WIN, LANES), 0)
        lane = iota((WIN, LANES), 1)
        near_map, far_map = table_maps(span, 2 * LANES)
        padded[...] = jnp.zeros_like(padded)
        padded[:heads, : span * span] = jax.nn.sigmoid(logits[...]) * (BIAS_RANGE * LOG2_E)
        table = padded[...]
        first = table.astype(BF16)
        second, third = split(table - first.astype(F32))
        table_a = dot_nn(first, near_map) + (dot_nn(second, near_map) + dot_nn(third, near_map))
        table_b = dot_nn(first, far_map) + (dot_nn(second, far_map) + dot_nn(third, far_map))
        for h in range(heads):
            near = jnp.broadcast_to(table_a[h : h + 1, :], (WIN, LANES))
            far = jnp.broadcast_to(table_b[h : h + 1, :], (WIN, LANES))
            near = pltpu.roll(near, LANES - WIN + 1, 1, stride=1, stride_axis=0)
            far = pltpu.roll(far, 1, 1, stride=1, stride_axis=0)
            line = jnp.where(lane % WIN <= sub, near, far)
            for r in range(WIN):
                one = pltpu.roll(line, (LANES - (WIN - 1 - r) * WIN) % LANES, 1)
                two = pltpu.roll(line, (LANES + TOKENS - (WIN - 1 - r) * WIN) % LANES, 1)
                at = h * TOKENS + r * WIN
                bias[at : at + WIN, :] = jnp.where(half, one, two)

        key = iota((TOKENS, LANES), 0)
        query = iota((TOKENS, LANES), 1) % TOKENS
        split_r = ((key // WIN) >= edge) != ((query // WIN) >= edge)
        split_c = ((key % WIN) >= edge) != ((query % WIN) >= edge)
        split_c = jnp.logical_and(split_c, iota((TOKENS, LANES), 1) >= TOKENS)
        mask_r = jnp.where(split_r, MASK_FILL * LOG2_E, 0.0)
        mask_c = jnp.where(split_c, MASK_FILL * LOG2_E, 0.0)

        def beside(ref, at, tile):
            one = ref[pl.ds(at, TOKENS), tile]
            two = ref[pl.ds(at + TOKENS, TOKENS), tile]
            return jnp.concatenate([one, two], axis=1)

        def stack(block):
            return jnp.concatenate([block * head_low[h] for h in range(per_tile)], axis=0)

        def diagonal(ref, at, tile):
            block = ref[pl.ds(at, pair), tile]
            return jnp.concatenate([block * top_rows, block * low_rows], axis=1)

        def turned(ref, at, tile):
            block = ref[pl.ds(at, pair), tile].T
            return jnp.concatenate([block * left_lanes, block * right_lanes], axis=0)

        def gather_heads(out):
            total = out[:TOKENS]
            for h in range(1, per_tile):
                total = jnp.where(owner == h, out[h * TOKENS : (h + 1) * TOKENS], total)
            return total

        tiles = [(p, g) for p in range(pairs) for g in range(groups)]

        def lanes_of(g):
            return slice(g * LANES, (g + 1) * LANES)

        def score(p, g):
            keys = stack(beside(k_hi, p * pair, lanes_of(g)))
            keys_low = stack(beside(k_lo, p * pair, lanes_of(g)))
            queries = turned(q_low, p * pair, lanes_of(g))
            raw[p, g] = dot_nn(keys, queries) + dot_nn(keys_low, queries)

        def soften(p, g):
            masks = []
            if p // pairs_across == row_windows - 1:
                masks.append(mask_r * last_row.astype(F32))
            if p % pairs_across == pairs_across - 1:
                masks.append(mask_c * last_col.astype(F32))
            for h in range(per_tile):
                place = slice(h * TOKENS, (h + 1) * TOKENS)
                head = g * per_tile + h
                line = q_turn[p, head * head_dim : head * head_dim + 1, :] * LOG2_E
                added = bias[head * TOKENS : (head + 1) * TOKENS, :]
                if masks:
                    added = added + functools.reduce(jnp.minimum, masks)
                s = raw[p, g, place, :] * line + added
                e = jnp.exp2(s - jnp.max(s, axis=0, keepdims=True))
                pr = e * (1.0 / jnp.sum(e, axis=0, keepdims=True))
                prob[p, g, place, :] = pr
                prob_low[p, g, place, :] = pr.astype(BF16)

        def attend(p, g):
            at, tile = p * pair, lanes_of(g)
            out = dot_tn(prob_low[p, g], stack(beside(val, at, tile)))
            att[at : at + TOKENS, tile] = out[:TOKENS, :LANES].astype(BF16)
            att[at + TOKENS : at + pair, tile] = out[TOKENS:, LANES:].astype(BF16)

        pipeline(tiles, (score, soften, attend))

        gains = gain[...].reshape(1, depth)

        def norm(p, d_gain):
            place = pl.ds(p * pair, pair)
            proj = dot_nn(att[place, :], w_proj[...])
            centre = proj - jnp.mean(proj, -1, keepdims=True)
            std = lax.rsqrt(jnp.mean(centre * centre, -1, keepdims=True) + EPS_NORM)
            normed = centre * std
            up = uf[place, :]
            d_gain = d_gain + jnp.sum(up * normed, axis=0, keepdims=True)
            u = up * gains
            d_p = std * (
                u - jnp.mean(u, -1, keepdims=True) - normed * jnp.mean(u * normed, -1, keepdims=True)
            )
            d_p = d_p.astype(BF16)
            d_prj[place, :] = d_p
            return d_gain

        d_gain = repeat(pairs, norm, jnp.zeros((1, depth), F32))

        w_proj_turned = w_proj[...].T

        def spread(p, carry):
            place = pl.ds(p * pair, pair)
            d_att[place, :] = dot_nn(d_prj[place, :], w_proj_turned).astype(BF16)
            return carry

        repeat(pairs, spread)

        def rise(p, g):
            values = stack(beside(val, p * pair, lanes_of(g)))
            d_prob[p, g] = dot_nn(values, turned(d_att, p * pair, lanes_of(g)))

        def harden(p, g):
            for h in range(per_tile):
                place = slice(h * TOKENS, (h + 1) * TOKENS)
                head = g * per_tile + h
                of = slice(head * TOKENS, (head + 1) * TOKENS)
                pr = prob[p, g, place, :]
                pd = pr * d_prob[p, g, place, :]
                d_s = pd - pr * jnp.sum(pd, axis=0, keepdims=True)
                if p == 0:
                    d_bias[of, :] = d_s
                else:
                    d_bias[of, :] += d_s
                d_s = d_s * q_turn[p, head * head_dim : head * head_dim + 1, :]
                by_scale = (d_s * raw[p, g, place, :]).reshape(WIN, WIN, LANES)
                of = slice(head * WIN, (head + 1) * WIN)
                if p == 0:
                    d_sc[of, :] = jnp.sum(by_scale, axis=0)
                else:
                    d_sc[of, :] += jnp.sum(by_scale, axis=0)
                d_low[p, g, place, :] = d_s.astype(BF16)

        def fall(p, g):
            at, tile = p * pair, lanes_of(g)
            key_tile = slice(depth + g * LANES, depth + (g + 1) * LANES)
            val_tile = slice(2 * depth + g * LANES, 2 * depth + (g + 1) * LANES)
            d_v = gather_heads(dot_nn(prob_low[p, g], diagonal(d_att, at, tile))).astype(BF16)
            d_qkv[at : at + TOKENS, val_tile] = d_v[:, :LANES]
            d_qkv[at + TOKENS : at + pair, val_tile] = d_v[:, LANES:]
            d_k = gather_heads(dot_nn(d_low[p, g], diagonal(q_low, at, tile)))
            d_unit[at : at + TOKENS, key_tile] = d_k[:, :LANES]
            d_unit[at + TOKENS : at + pair, key_tile] = d_k[:, LANES:]
            d_q = dot_tn(d_low[p, g], stack(beside(k_hi, at, tile)))
            d_unit[at : at + TOKENS, tile] = d_q[:TOKENS, :LANES]
            d_unit[at + TOKENS : at + pair, tile] = d_q[TOKENS:, LANES:]

        pipeline(tiles, (rise, harden, fall))

        w_qkv_turned = w_qkv[...].T

        def flatten(p, carry):
            place = pl.ds(p * pair, pair)
            unit = unit_s[place, :]
            d_u = d_unit[place, :]
            d_u = d_u - unit * group_sum(unit * d_u, ones, False)
            d_qkv[place, :depth] = d_u[:, :depth].astype(BF16)
            d_qkv[place, depth : 2 * depth] = (inv[place, :] * d_u[:, depth:]).astype(BF16)
            flat = dot_nn(d_qkv[place, :], w_qkv_turned)
            for w in range(2):
                i0 = p // pairs_across * WIN
                j0 = (p % pairs_across * 2 + w) * WIN
                for r in range(WIN):
                    piece = flat[w * TOKENS + r * WIN : w * TOKENS + (r + 1) * WIN]
                    d_img[i0 + r, pl.ds(j0, WIN), :] = piece.astype(BF16)
            return carry

        repeat(pairs, flatten)

        d_wp = dot_tn(d_prj[...], att[...])
        d_wq = dot_tn(d_qkv[...], xb[...])
        for b in range(2):
            for j in range(groups):
                tile = slice(j * LANES, (j + 1) * LANES)
                at = b * sent_rows + j * body
                sums[at : at + half_q, :] = d_wq[b * half_q : (b + 1) * half_q, tile].astype(BF16)
                at = at + half_q
                sums[at : at + half_p, :] = d_wp[b * half_p : (b + 1) * half_p, tile].astype(BF16)

        small[...] = jnp.zeros_like(small)
        for h in range(heads):
            line = jnp.zeros((WIN, LANES), F32)
            for r in range(WIN):
                at = h * TOKENS + r * WIN
                part = d_bias[at : at + WIN, :]
                part = jnp.where(half, part + pltpu.roll(part, TOKENS, 1), 0.0)
                line = line + pltpu.roll(part, (WIN - 1 - r) * WIN, 1)
            near, far = jnp.zeros_like(line), jnp.zeros_like(line)
            for c in range(WIN):
                own = jnp.where(sub == c, line, 0.0)
                near = near + pltpu.roll(own, WIN - 1 - c, 1)
                far = far + pltpu.roll(own, LANES - 1 - c, 1)
            near = jnp.where(lane % WIN >= WIN - 1 - sub, near, 0.0)
            far = jnp.where(lane % WIN + sub + 1 <= WIN - 1, far, 0.0)
            small[h : h + 1, :] = jnp.sum(near, axis=0, keepdims=True)
            small[heads + h : heads + h + 1, :] = jnp.sum(far, axis=0, keepdims=True)
        for j in range(groups):
            small[2 * heads + j : 2 * heads + j + 1, :] = d_gain[:, j * LANES : (j + 1) * LANES]
        line = jnp.zeros((1, LANES), F32)
        for h in range(heads):
            total = jnp.sum(d_sc[h * WIN : (h + 1) * WIN, :], axis=0, keepdims=True)
            total = jnp.sum(total, axis=1, keepdims=True)
            line = line + jnp.where(iota((1, LANES), 1) == h, total, 0.0)
        at = 2 * heads + groups
        small[at : at + 1, :] = line
        for b in range(2):
            at = b * sent_rows + small_at
            sums[at : at + small_rows, :] = small[...].astype(BF16)
        for out, whose in ((mine, core), (given, 1 - core)):
            turn = whose if crossed else 0
            for f in range(outer):
                for n in range(inner):
                    image = f + (n - f) * turn
                    column = n + (f - n) * turn
                    at = image * sent_rows + whose * core_rows + column * chunk
                    out[f, n] = sums[pl.ds(pl.multiple_of(at, 8), chunk), :]

    def call(limit, tok, cot, below, right, corner, w_qkv, w_proj, logits, gain):
        vmem = pltpu.VMEM
        scratch = [
            vmem((tokens, depth), BF16),
            vmem((tokens, depth), F32),
            vmem((tokens, 2 * depth), F32),
            vmem((tokens, depth), F32),
            vmem((tokens, depth), BF16),
            vmem((pairs, depth, pair), F32),
            vmem((tokens, depth), BF16),
            vmem((tokens, depth), BF16),
            vmem((tokens, depth), BF16),
            vmem((pairs, groups, stacked, LANES), F32),
            vmem((pairs, groups, stacked, LANES), BF16),
            vmem((pairs, groups, stacked, LANES), F32),
            vmem((pairs, groups, stacked, LANES), F32),
            vmem((pairs, groups, stacked, LANES), BF16),
            vmem((tokens, depth), BF16),
            vmem((tokens, depth), BF16),
            vmem((tokens, depth), BF16),
            vmem((tokens, 3 * depth), BF16),
            vmem((tokens, 2 * depth), F32),
            vmem((heads * TOKENS, LANES), F32),
            vmem((heads * TOKENS, LANES), F32),
            vmem((heads * WIN, LANES), F32),
            vmem((small_rows, LANES), F32),
            vmem((2 * sent_rows, LANES), BF16),
            vmem((16, 2 * LANES), F32),
            vmem((groups, rows * pitch, LANES), F32),
            vmem((groups, rows * pitch, LANES), F32),
        ]
        part = jax.ShapeDtypeStruct((outer, inner, chunk, LANES), BF16)
        return pl.pallas_call(
            kernel,
            out_shape=(jax.ShapeDtypeStruct((rows, cols, depth), BF16), part, part),
            in_specs=[pl.BlockSpec(memory_space=pltpu.SMEM)]
            + [pl.BlockSpec(memory_space=pltpu.VMEM)] * 9,
            out_specs=tuple([pl.BlockSpec(memory_space=pltpu.VMEM)] * 3),
            scratch_shapes=scratch,
            compiler_params=pltpu.CompilerParams(vmem_limit_bytes=VMEM_MAIN),
            name="block_grads",
        )(limit, tok, cot, below, right, corner, w_qkv, w_proj, logits, gain)

    return call


def finish(ours, theirs, logits, limit, depth, heads):
    core_rows = ours.shape[0]
    groups = depth // LANES
    half_q = 3 * depth // 2
    half_p = depth // 2
    body = half_q + half_p
    small_at = groups * body
    span = 2 * WIN - 1

    def kernel(limit, ours, theirs, logits, d_wq, d_wp, d_table, d_scale, d_gain, whole):
        core = lax.axis_index("hc")
        whole[pl.ds(pl.multiple_of(core * core_rows, 8), core_rows), :] = ours[...].astype(F32)
        other = pl.multiple_of((1 - core) * core_rows, 8)
        whole[pl.ds(other, core_rows), :] = theirs[...].astype(F32)
        for j in range(groups):
            tile = slice(j * LANES, (j + 1) * LANES)
            d_wq[:, tile] = whole[j * body : j * body + half_q, :]
            d_wp[:, tile] = whole[j * body + half_q : (j + 1) * body, :]
        small = whole[small_at : small_at + 32, :]
        near_map, far_map = table_maps(span, 2 * LANES)
        table = dot_nt(small[:16].astype(BF16), near_map)
        table = table + dot_nt(small[heads : heads + 16].astype(BF16), far_map)
        table = table[:heads, : span * span]
        sigma = jax.nn.sigmoid(logits[...])
        d_table[...] = table * (BIAS_RANGE * sigma * (1.0 - sigma))
        gains = [small[2 * heads + j : 2 * heads + j + 1, :] for j in range(groups)]
        d_gain[...] = jnp.concatenate(gains, axis=1).reshape(depth)
        lane = iota((1, LANES), 1)
        kept = jnp.zeros((1, LANES), F32)
        for h in range(heads):
            kept = jnp.where(lane == h, jnp.where(limit[h] < SCALE_CAP, 1.0, 0.0), kept)
        row = small[2 * heads + groups : 2 * heads + groups + 1, :] * kept
        d_scale[...] = row[:, :heads].reshape(heads)

    vmem = pl.BlockSpec(memory_space=pltpu.VMEM)
    return pl.pallas_call(
        kernel,
        out_shape=(
            jax.ShapeDtypeStruct((half_q, depth), F32),
            jax.ShapeDtypeStruct((half_p, depth), F32),
            jax.ShapeDtypeStruct(logits.shape, F32),
            jax.ShapeDtypeStruct((heads,), F32),
            jax.ShapeDtypeStruct((depth,), F32),
        ),
        in_specs=[pl.BlockSpec(memory_space=pltpu.SMEM), vmem, vmem, vmem],
        out_specs=(vmem,) * 5,
        scratch_shapes=[pltpu.VMEM((2 * core_rows, LANES), F32)],
        compiler_params=pltpu.CompilerParams(vmem_limit_bytes=VMEM_LAST),
        name="finish",
    )(limit, ours, theirs, logits)


def route(axes, move):
    sizes = [lax.axis_size(a) for a in axes]
    pairs = []
    for flat in range(math.prod(sizes)):
        left, where = flat, []
        for size in reversed(sizes):
            where.append(left % size)
            left //= size
        where = move(where[::-1], sizes)
        target = 0
        for place, size in zip(where, sizes):
            target = target * size + place
        pairs.append((flat, target))
    return pairs


GRID = ("hz", "hc", "wa")


def step(rows, cols):
    def move(where, sizes):
        high = (where[0] * sizes[1] + where[1] + rows) % (sizes[0] * sizes[1])
        return [high // sizes[1], high % sizes[1], (where[2] + cols) % sizes[2]]

    return move


FACE = ("hc", "wa", "ba")


def over(turn, by, crossed):
    def move(where, sizes):
        axis = 2 - (turn + (where[0] if crossed else 0)) % 2
        where = list(where)
        where[axis] = (where[axis] + by) % sizes[axis]
        return where

    return move


def along(by):
    return lambda where, sizes: [(where[0] + by) % sizes[0]]


def hand_out(blocks, place, axes, move):
    count = blocks.shape[0]
    total = lax.dynamic_index_in_dim(blocks, place, 0, keepdims=False).astype(F32)
    for by in range(count - 1, 0, -1):
        sent = lax.dynamic_index_in_dim(blocks, (place + by) % count, 0, keepdims=False)
        total = total + lax.ppermute(sent, axes, route(axes, move(by))).astype(F32)
    return total.astype(BF16)


def shards(tokens, cotangent, w_qkv, w_proj, table_logits, logit_scale, gain):
    images, rows, cols, depth = tokens.shape
    heads = logit_scale.shape[0]
    edge = WIN // 2
    both = jnp.concatenate([tokens, cotangent], 0)
    top = both[:, :edge]
    left = both[:, edge:, :edge].reshape(2, (rows - edge) * edge, depth)
    tip = both[:, :edge, :edge].reshape(2, edge * edge, depth)
    below = lax.ppermute(top, GRID, route(GRID, step(-1, 0)))
    right = lax.ppermute(left, GRID, route(GRID, step(0, -1)))
    corner = lax.ppermute(tip, GRID, route(GRID, step(-1, -1)))

    cores, tall, across = lax.axis_size("hc"), lax.axis_size("hz"), lax.axis_size("wa")
    images_over = lax.axis_size("ba")
    owners = cores * tall * across
    used = 2 * depth // LANES * depth + 2 * heads + depth // LANES + 1
    unit = 8 * owners
    sent = -(-used // unit) * unit
    crossed = images_over == across
    order = (images_over, across, crossed)
    call = make_kernel(rows, cols, depth, heads, sent, across, order)
    d_moved, mine, given = call(
        logit_scale, tokens, cotangent, below, right, corner, w_qkv, w_proj, table_logits, gain
    )

    right = lax.ppermute(d_moved[: rows - edge, cols - edge :], GRID, route(GRID, step(0, 1)))
    lower = lax.ppermute(d_moved[rows - edge :, : cols - edge], GRID, route(GRID, step(1, 0)))
    cross = lax.ppermute(
        d_moved[rows - edge :, cols - edge :], GRID, route(GRID, step(1, 1))
    )
    upper = jnp.concatenate([cross, lower], 1)
    main = jnp.concatenate([right, d_moved[: rows - edge, : cols - edge]], 1)
    back = jnp.concatenate([upper, main], 0)[None]
    d_tokens = (cotangent.astype(F32) + back.astype(F32)).astype(BF16)

    swap = route(("hc",), lambda where, sizes: [1 - where[0]])
    one = jnp.where(lax.axis_index("hc") < 0, 0.0, 1.0).astype(BF16)
    taken = lax.ppermute(given * one, "hc", swap)
    summed = (mine.astype(F32) + taken.astype(F32)).astype(BF16)
    piece = sent // owners
    core, column, image = lax.axis_index("hc"), lax.axis_index("wa"), lax.axis_index("ba")
    turn = core if crossed else 0
    moves = (lambda by: over(0, by, crossed)), (lambda by: over(1, by, crossed))
    summed = hand_out(summed, image + (column - image) * turn, FACE, moves[0])
    summed = hand_out(summed, column + (image - column) * turn, FACE, moves[1])
    summed = summed.reshape(tall, piece, LANES)
    total = hand_out(summed, lax.axis_index("hz"), ("hz",), along)
    spread = jnp.broadcast_to(total[None], (tall * across, piece, LANES))
    ours = lax.all_to_all(spread, ("wa", "hz"), 0, 0, tiled=True)
    ours = ours.reshape(sent // cores, LANES)
    theirs = lax.ppermute(ours, "hc", swap)
    d_wq, d_wp, d_table, d_scale, d_gain = finish(
        ours, theirs, table_logits, logit_scale, depth, heads
    )
    return (d_tokens, d_wq.T, d_wp.T, d_table, d_scale, d_gain)


def solution(mesh):
    sizes = mesh.shape
    devices = mesh.devices.reshape(sizes["ha"] // 2, 2, sizes["wa"], sizes["ba"])
    inner = Mesh(devices, ("hz", "hc", "wa", "ba"))
    image = P("ba", ("hz", "hc"), "wa", None)
    return jax.shard_map(
        shards,
        mesh=inner,
        in_specs=(image, image, P(), P(), P(), P(), P()),
        out_specs=(image, P(None, "ba"), P(None, "ba"), P(), P(), P()),
        check_vma=False,
    )
```

```python
import functools
import math

import jax
import jax.numpy as jnp
from jax import lax
from jax.experimental import pallas as pl
from jax.experimental.pallas import tpu as pltpu
from jax.sharding import Mesh
from jax.sharding import PartitionSpec as P

WIN = 8
TOKENS = WIN * WIN
LANES = 128
EPS_NORM = 1e-05
MASK_FILL = -100.0
SCALE_CAP = math.log(100.0)
BIAS_RANGE = 16.0
LOG2_E = math.log2(math.e)
VMEM_MAIN = 36 << 20
VMEM_LAST = 12 << 20
F32 = jnp.float32
BF16 = jnp.bfloat16


def dot_nn(left, right):
    return lax.dot_general(left, right, (((1,), (0,)), ((), ())), preferred_element_type=F32)


def dot_nt(left, right):
    return lax.dot_general(left, right, (((1,), (1,)), ((), ())), preferred_element_type=F32)


def dot_tn(left, right):
    return lax.dot_general(left, right, (((0,), (0,)), ((), ())), preferred_element_type=F32)


def iota(shape, dim):
    return lax.broadcasted_iota(jnp.int32, shape, dim)


def split(value):
    high = value.astype(BF16)
    return high, (value - high.astype(F32)).astype(BF16)


def group_sum(value, ones, fine=True):
    high, low = split(value)
    width = ones.shape[0]
    parts = []
    for start in range(0, value.shape[1], width):
        part = slice(start, start + width)
        total = dot_nn(high[:, part], ones)
        parts.append(total + dot_nn(low[:, part], ones) if fine else total)
    return jnp.concatenate(parts, axis=1)


def table_maps(span, used):
    entry = iota((used, LANES), 0)
    lane = iota((used, LANES), 1)
    same_row = entry // span == lane // WIN
    near = jnp.logical_and(same_row, entry % span == lane % WIN)
    far = jnp.logical_and(same_row, entry % span == lane % WIN + WIN)
    return near.astype(F32).astype(BF16), far.astype(F32).astype(BF16)


def repeat(count, step, carry=0):
    for p in range(count):
        carry = step(p, carry)
    return carry


def pipeline(items, stages):
    for start in range(len(items) + len(stages)):
        for back, stage in zip((0, 2, 3), stages):
            if 0 <= start - back < len(items):
                stage(*items[start - back])


def make_kernel(rows, cols, depth, heads, sent_rows, across, order):
    head_dim = depth // heads
    per_tile = LANES // head_dim
    groups = heads // per_tile
    col_windows = cols // WIN
    row_windows = rows // WIN
    pairs = row_windows * col_windows // 2
    pairs_across = col_windows // 2
    stacked = per_tile * TOKENS
    pair = 2 * TOKENS
    tokens = rows * cols
    span = 2 * WIN - 1
    half_q = 3 * depth // 2
    half_p = depth // 2
    body = half_q + half_p
    small_at = groups * body
    small_rows = sent_rows - small_at
    core_rows = sent_rows // 2
    edge = WIN // 2
    pitch = cols + WIN
    outer, inner, crossed = order
    chunk = core_rows // across

    def kernel(
        limit,
        tok,
        cot,
        below,
        right,
        corner,
        w_qkv,
        w_proj,
        logits,
        gain,
        d_img,
        mine,
        given,
        xb,
        uf,
        unit_s,
        inv,
        q_low,
        q_turn,
        k_hi,
        k_lo,
        val,
        prob,
        prob_low,
        raw,
        d_prob,
        d_low,
        att,
        d_prj,
        d_att,
        d_qkv,
        d_unit,
        bias,
        d_bias,
        d_sc,
        small,
        sums,
        padded,
        wide_x,
        wide_u,
    ):
        core = lax.axis_index("hc")
        down = lax.axis_index("hz") * lax.axis_size("hc") + core
        last_row = (down == lax.axis_size("hz") * lax.axis_size("hc") - 1).astype(jnp.int32)
        last_col = (lax.axis_index("wa") == lax.axis_size("wa") - 1).astype(jnp.int32)
        half = iota((1, LANES), 1) < TOKENS
        wide = 2 * LANES
        ones = (iota((wide, wide), 0) // head_dim == iota((wide, wide), 1) // head_dim).astype(F32)
        ones = ones.astype(BF16)
        owner = iota((1, wide), 1) % LANES // head_dim
        head_low = [(owner == h).astype(F32).astype(BF16) for h in range(per_tile)]
        top_rows = (iota((pair, LANES), 0) < TOKENS).astype(F32)
        top_rows, low_rows = top_rows.astype(BF16), (1.0 - top_rows).astype(BF16)
        left_lanes = half.astype(F32)
        left_lanes, right_lanes = left_lanes.astype(BF16), (1.0 - left_lanes).astype(BF16)
        by_head = iota((1, depth), 1) // head_dim
        scale = jnp.zeros((1, depth), F32)
        for h in range(heads):
            scale = jnp.where(by_head == h, limit[h], scale)
        scale = jnp.exp(jnp.minimum(scale, SCALE_CAP))

        for which, (own, wide_of) in enumerate(((tok, wide_x), (cot, wide_u))):
            edges = right[which].astype(F32)
            ends = corner[which].astype(F32)
            for i in range(rows):
                if i + edge < rows:
                    row = own[0, i + edge].astype(F32)
                    side = edges[i * edge : (i + 1) * edge]
                else:
                    row = below[which, i + edge - rows].astype(F32)
                    side = ends[(i + edge - rows) * edge : (i + edge - rows + 1) * edge]
                at = i * pitch
                for j in range(groups):
                    tile = slice(j * LANES, (j + 1) * LANES)
                    wide_of[j, at : at + cols, :] = row[:, tile]
                    wide_of[j, at + cols : at + cols + edge, :] = side[:, tile]

        def window_rows(wide_of, p):
            tiles = []
            for j in range(groups):
                pieces = []
                for w in range(2):
                    i0 = p // pairs_across * WIN
                    j0 = (p % pairs_across * 2 + w) * WIN + edge
                    for r in range(WIN):
                        at = (i0 + r) * pitch + j0
                        pieces.append(wide_of[j, at : at + WIN, :])
                tiles.append(jnp.concatenate(pieces, axis=0))
            return jnp.concatenate(tiles, axis=1)

        def project(p, carry):
            place = pl.ds(p * pair, pair)
            x = window_rows(wide_x, p).astype(BF16)
            uf[place, :] = window_rows(wide_u, p)
            xb[place, :] = x
            qkv = dot_nn(x, w_qkv[...]).astype(BF16)
            val[place, :] = qkv[:, 2 * depth :]
            both = qkv[:, : 2 * depth].astype(F32)
            root = lax.rsqrt(group_sum(both * both, ones) + 1.0)
            unit = both * root
            unit_s[place, :] = unit
            inv[place, :] = root[:, depth:]
            q_low[place, :] = qkv[:, :depth]
            q_turn[p] = (root[:, :depth] * scale).T
            k_hi[place, :], k_lo[place, :] = split(unit[:, depth:])
            return carry

        repeat(pairs, project)

        sub = iota((WIN, LANES), 0)
        lane = iota((WIN, LANES), 1)
        near_map, far_map = table_maps(span, 2 * LANES)
        padded[...] = jnp.zeros_like(padded)
        padded[:heads, : span * span] = jax.nn.sigmoid(logits[...]) * (BIAS_RANGE * LOG2_E)
        table = padded[...]
        first = table.astype(BF16)
        second, third = split(table - first.astype(F32))
        table_a = dot_nn(first, near_map) + (dot_nn(second, near_map) + dot_nn(third, near_map))
        table_b = dot_nn(first, far_map) + (dot_nn(second, far_map) + dot_nn(third, far_map))
        for h in range(heads):
            near = jnp.broadcast_to(table_a[h : h + 1, :], (WIN, LANES))
            far = jnp.broadcast_to(table_b[h : h + 1, :], (WIN, LANES))
            near = pltpu.roll(near, LANES - WIN + 1, 1, stride=1, stride_axis=0)
            far = pltpu.roll(far, 1, 1, stride=1, stride_axis=0)
            line = jnp.where(lane % WIN <= sub, near, far)
            for r in range(WIN):
                one = pltpu.roll(line, (LANES - (WIN - 1 - r) * WIN) % LANES, 1)
                two = pltpu.roll(line, (LANES + TOKENS - (WIN - 1 - r) * WIN) % LANES, 1)
                at = h * TOKENS + r * WIN
                bias[at : at + WIN, :] = jnp.where(half, one, two)

        key = iota((TOKENS, LANES), 0)
        query = iota((TOKENS, LANES), 1) % TOKENS
        split_r = ((key // WIN) >= edge) != ((query // WIN) >= edge)
        split_c = ((key % WIN) >= edge) != ((query % WIN) >= edge)
        split_c = jnp.logical_and(split_c, iota((TOKENS, LANES), 1) >= TOKENS)
        mask_r = jnp.where(split_r, MASK_FILL * LOG2_E, 0.0)
        mask_c = jnp.where(split_c, MASK_FILL * LOG2_E, 0.0)

        def beside(ref, at, tile):
            one = ref[pl.ds(at, TOKENS), tile]
            two = ref[pl.ds(at + TOKENS, TOKENS), tile]
            return jnp.concatenate([one, two], axis=1)

        def stack(block):
            return jnp.concatenate([block * head_low[h] for h in range(per_tile)], axis=0)

        def diagonal(ref, at, tile):
            block = ref[pl.ds(at, pair), tile]
            return jnp.concatenate([block * top_rows, block * low_rows], axis=1)

        def turned(ref, at, tile):
            block = ref[pl.ds(at, pair), tile].T
            return jnp.concatenate([block * left_lanes, block * right_lanes], axis=0)

        def gather_heads(out):
            total = out[:TOKENS]
            for h in range(1, per_tile):
                total = jnp.where(owner == h, out[h * TOKENS : (h + 1) * TOKENS], total)
            return total

        tiles = [(p, g) for p in range(pairs) for g in range(groups)]

        def lanes_of(g):
            return slice(g * LANES, (g + 1) * LANES)

        def score(p, g):
            keys = stack(beside(k_hi, p * pair, lanes_of(g)))
            keys_low = stack(beside(k_lo, p * pair, lanes_of(g)))
            queries = turned(q_low, p * pair, lanes_of(g))
            raw[p, g] = dot_nn(keys, queries) + dot_nn(keys_low, queries)

        def soften(p, g):
            masks = []
            if p // pairs_across == row_windows - 1:
                masks.append(mask_r * last_row.astype(F32))
            if p % pairs_across == pairs_across - 1:
                masks.append(mask_c * last_col.astype(F32))
            for h in range(per_tile):
                place = slice(h * TOKENS, (h + 1) * TOKENS)
                head = g * per_tile + h
                line = q_turn[p, head * head_dim : head * head_dim + 1, :] * LOG2_E
                added = bias[head * TOKENS : (head + 1) * TOKENS, :]
                if masks:
                    added = added + functools.reduce(jnp.minimum, masks)
                s = raw[p, g, place, :] * line + added
                e = jnp.exp2(s - jnp.max(s, axis=0, keepdims=True))
                pr = e * (1.0 / jnp.sum(e, axis=0, keepdims=True))
                prob[p, g, place, :] = pr
                prob_low[p, g, place, :] = pr.astype(BF16)

        def attend(p, g):
            at, tile = p * pair, lanes_of(g)
            out = dot_tn(prob_low[p, g], stack(beside(val, at, tile)))
            att[at : at + TOKENS, tile] = out[:TOKENS, :LANES].astype(BF16)
            att[at + TOKENS : at + pair, tile] = out[TOKENS:, LANES:].astype(BF16)

        pipeline(tiles, (score, soften, attend))

        gains = gain[...].reshape(1, depth)

        def norm(p, d_gain):
            place = pl.ds(p * pair, pair)
            proj = dot_nn(att[place, :], w_proj[...])
            centre = proj - jnp.mean(proj, -1, keepdims=True)
            std = lax.rsqrt(jnp.mean(centre * centre, -1, keepdims=True) + EPS_NORM)
            normed = centre * std
            up = uf[place, :]
            d_gain = d_gain + jnp.sum(up * normed, axis=0, keepdims=True)
            u = up * gains
            d_p = std * (
                u - jnp.mean(u, -1, keepdims=True) - normed * jnp.mean(u * normed, -1, keepdims=True)
            )
            d_p = d_p.astype(BF16)
            d_prj[place, :] = d_p
            return d_gain

        d_gain = repeat(pairs, norm, jnp.zeros((1, depth), F32))

        w_proj_turned = w_proj[...].T

        def spread(p, carry):
            place = pl.ds(p * pair, pair)
            d_att[place, :] = dot_nn(d_prj[place, :], w_proj_turned).astype(BF16)
            return carry

        repeat(pairs, spread)

        def rise(p, g):
            values = stack(beside(val, p * pair, lanes_of(g)))
            d_prob[p, g] = dot_nn(values, turned(d_att, p * pair, lanes_of(g)))

        def harden(p, g):
            for h in range(per_tile):
                place = slice(h * TOKENS, (h + 1) * TOKENS)
                head = g * per_tile + h
                of = slice(head * TOKENS, (head + 1) * TOKENS)
                pr = prob[p, g, place, :]
                pd = pr * d_prob[p, g, place, :]
                d_s = pd - pr * jnp.sum(pd, axis=0, keepdims=True)
                if p == 0:
                    d_bias[of, :] = d_s
                else:
                    d_bias[of, :] += d_s
                d_s = d_s * q_turn[p, head * head_dim : head * head_dim + 1, :]
                by_scale = (d_s * raw[p, g, place, :]).reshape(WIN, WIN, LANES)
                of = slice(head * WIN, (head + 1) * WIN)
                if p == 0:
                    d_sc[of, :] = jnp.sum(by_scale, axis=0)
                else:
                    d_sc[of, :] += jnp.sum(by_scale, axis=0)
                d_low[p, g, place, :] = d_s.astype(BF16)

        def fall(p, g):
            at, tile = p * pair, lanes_of(g)
            key_tile = slice(depth + g * LANES, depth + (g + 1) * LANES)
            val_tile = slice(2 * depth + g * LANES, 2 * depth + (g + 1) * LANES)
            d_v = gather_heads(dot_nn(prob_low[p, g], diagonal(d_att, at, tile))).astype(BF16)
            d_qkv[at : at + TOKENS, val_tile] = d_v[:, :LANES]
            d_qkv[at + TOKENS : at + pair, val_tile] = d_v[:, LANES:]
            d_k = gather_heads(dot_nn(d_low[p, g], diagonal(q_low, at, tile)))
            d_unit[at : at + TOKENS, key_tile] = d_k[:, :LANES]
            d_unit[at + TOKENS : at + pair, key_tile] = d_k[:, LANES:]
            d_q = dot_tn(d_low[p, g], stack(beside(k_hi, at, tile)))
            d_unit[at : at + TOKENS, tile] = d_q[:TOKENS, :LANES]
            d_unit[at + TOKENS : at + pair, tile] = d_q[TOKENS:, LANES:]

        pipeline(tiles, (rise, harden, fall))

        w_qkv_turned = w_qkv[...].T

        def flatten(p, carry):
            place = pl.ds(p * pair, pair)
            unit = unit_s[place, :]
            d_u = d_unit[place, :]
            d_u = d_u - unit * group_sum(unit * d_u, ones, False)
            d_qkv[place, :depth] = d_u[:, :depth].astype(BF16)
            d_qkv[place, depth : 2 * depth] = (inv[place, :] * d_u[:, depth:]).astype(BF16)
            flat = dot_nn(d_qkv[place, :], w_qkv_turned)
            for w in range(2):
                i0 = p // pairs_across * WIN
                j0 = (p % pairs_across * 2 + w) * WIN
                for r in range(WIN):
                    piece = flat[w * TOKENS + r * WIN : w * TOKENS + (r + 1) * WIN]
                    d_img[i0 + r, pl.ds(j0, WIN), :] = piece.astype(BF16)
            return carry

        repeat(pairs, flatten)

        d_wp = dot_tn(d_prj[...], att[...])
        d_wq = dot_tn(d_qkv[...], xb[...])
        for b in range(2):
            for j in range(groups):
                tile = slice(j * LANES, (j + 1) * LANES)
                at = b * sent_rows + j * body
                sums[at : at + half_q, :] = d_wq[b * half_q : (b + 1) * half_q, tile].astype(BF16)
                at = at + half_q
                sums[at : at + half_p, :] = d_wp[b * half_p : (b + 1) * half_p, tile].astype(BF16)

        small[...] = jnp.zeros_like(small)
        for h in range(heads):
            line = jnp.zeros((WIN, LANES), F32)
            for r in range(WIN):
                at = h * TOKENS + r * WIN
                part = d_bias[at : at + WIN, :]
                part = jnp.where(half, part + pltpu.roll(part, TOKENS, 1), 0.0)
                line = line + pltpu.roll(part, (WIN - 1 - r) * WIN, 1)
            near, far = jnp.zeros_like(line), jnp.zeros_like(line)
            for c in range(WIN):
                own = jnp.where(sub == c, line, 0.0)
                near = near + pltpu.roll(own, WIN - 1 - c, 1)
                far = far + pltpu.roll(own, LANES - 1 - c, 1)
            near = jnp.where(lane % WIN >= WIN - 1 - sub, near, 0.0)
            far = jnp.where(lane % WIN + sub + 1 <= WIN - 1, far, 0.0)
            small[h : h + 1, :] = jnp.sum(near, axis=0, keepdims=True)
            small[heads + h : heads + h + 1, :] = jnp.sum(far, axis=0, keepdims=True)
        for j in range(groups):
            small[2 * heads + j : 2 * heads + j + 1, :] = d_gain[:, j * LANES : (j + 1) * LANES]
        line = jnp.zeros((1, LANES), F32)
        for h in range(heads):
            total = jnp.sum(d_sc[h * WIN : (h + 1) * WIN, :], axis=0, keepdims=True)
            total = jnp.sum(total, axis=1, keepdims=True)
            line = line + jnp.where(iota((1, LANES), 1) == h, total, 0.0)
        at = 2 * heads + groups
        small[at : at + 1, :] = line
        for b in range(2):
            at = b * sent_rows + small_at
            sums[at : at + small_rows, :] = small[...].astype(BF16)
        for out, whose in ((mine, core), (given, 1 - core)):
            turn = whose if crossed else 0
            for f in range(outer):
                for n in range(inner):
                    image = f + (n - f) * turn
                    column = n + (f - n) * turn
                    at = image * sent_rows + whose * core_rows + column * chunk
                    out[f, n] = sums[pl.ds(pl.multiple_of(at, 8), chunk), :]

    def call(limit, tok, cot, below, right, corner, w_qkv, w_proj, logits, gain):
        vmem = pltpu.VMEM
        scratch = [
            vmem((tokens, depth), BF16),
            vmem((tokens, depth), F32),
            vmem((tokens, 2 * depth), F32),
            vmem((tokens, depth), F32),
            vmem((tokens, depth), BF16),
            vmem((pairs, depth, pair), F32),
            vmem((tokens, depth), BF16),
            vmem((tokens, depth), BF16),
            vmem((tokens, depth), BF16),
            vmem((pairs, groups, stacked, LANES), F32),
            vmem((pairs, groups, stacked, LANES), BF16),
            vmem((pairs, groups, stacked, LANES), F32),
            vmem((pairs, groups, stacked, LANES), F32),
            vmem((pairs, groups, stacked, LANES), BF16),
            vmem((tokens, depth), BF16),
            vmem((tokens, depth), BF16),
            vmem((tokens, depth), BF16),
            vmem((tokens, 3 * depth), BF16),
            vmem((tokens, 2 * depth), F32),
            vmem((heads * TOKENS, LANES), F32),
            vmem((heads * TOKENS, LANES), F32),
            vmem((heads * WIN, LANES), F32),
            vmem((small_rows, LANES), F32),
            vmem((2 * sent_rows, LANES), BF16),
            vmem((16, 2 * LANES), F32),
            vmem((groups, rows * pitch, LANES), F32),
            vmem((groups, rows * pitch, LANES), F32),
        ]
        part = jax.ShapeDtypeStruct((outer, inner, chunk, LANES), BF16)
        return pl.pallas_call(
            kernel,
            out_shape=(jax.ShapeDtypeStruct((rows, cols, depth), BF16), part, part),
            in_specs=[pl.BlockSpec(memory_space=pltpu.SMEM)]
            + [pl.BlockSpec(memory_space=pltpu.VMEM)] * 9,
            out_specs=tuple([pl.BlockSpec(memory_space=pltpu.VMEM)] * 3),
            scratch_shapes=scratch,
            compiler_params=pltpu.CompilerParams(vmem_limit_bytes=VMEM_MAIN),
            name="block_grads",
        )(limit, tok, cot, below, right, corner, w_qkv, w_proj, logits, gain)

    return call


def finish(ours, theirs, logits, limit, depth, heads):
    core_rows = ours.shape[0]
    groups = depth // LANES
    half_q = 3 * depth // 2
    half_p = depth // 2
    body = half_q + half_p
    small_at = groups * body
    span = 2 * WIN - 1

    def kernel(limit, ours, theirs, logits, d_wq, d_wp, d_table, d_scale, d_gain, whole, wq, wp, sems):
        core = lax.axis_index("hc")
        whole[pl.ds(pl.multiple_of(core * core_rows, 8), core_rows), :] = ours[...].astype(F32)
        other = pl.multiple_of((1 - core) * core_rows, 8)
        whole[pl.ds(other, core_rows), :] = theirs[...].astype(F32)
        copies = []
        for j in range(groups):
            tile = slice(j * LANES, (j + 1) * LANES)
            wq[:, tile] = whole[j * body : j * body + half_q, :]
            wp[:, tile] = whole[j * body + half_q : (j + 1) * body, :]
            for k, (src, dst) in enumerate(((wq, d_wq), (wp, d_wp))):
                copy = pltpu.make_async_copy(src.at[:, tile], dst.at[:, tile], sems.at[k, j])
                copy.start()
                copies.append(copy)
        small = whole[small_at : small_at + 32, :]
        near_map, far_map = table_maps(span, 2 * LANES)
        table = dot_nt(small[:16].astype(BF16), near_map)
        table = table + dot_nt(small[heads : heads + 16].astype(BF16), far_map)
        table = table[:heads, : span * span]
        sigma = jax.nn.sigmoid(logits[...])
        d_table[...] = table * (BIAS_RANGE * sigma * (1.0 - sigma))
        gains = [small[2 * heads + j : 2 * heads + j + 1, :] for j in range(groups)]
        d_gain[...] = jnp.concatenate(gains, axis=1).reshape(depth)
        lane = iota((1, LANES), 1)
        kept = jnp.zeros((1, LANES), F32)
        for h in range(heads):
            kept = jnp.where(lane == h, jnp.where(limit[h] < SCALE_CAP, 1.0, 0.0), kept)
        row = small[2 * heads + groups : 2 * heads + groups + 1, :] * kept
        d_scale[...] = row[:, :heads].reshape(heads)
        for copy in copies:
            copy.wait()

    vmem = pl.BlockSpec(memory_space=pltpu.VMEM)
    return pl.pallas_call(
        kernel,
        out_shape=(
            jax.ShapeDtypeStruct((half_q, depth), F32),
            jax.ShapeDtypeStruct((half_p, depth), F32),
            jax.ShapeDtypeStruct(logits.shape, F32),
            jax.ShapeDtypeStruct((heads,), F32),
            jax.ShapeDtypeStruct((depth,), F32),
        ),
        in_specs=[pl.BlockSpec(memory_space=pltpu.SMEM), vmem, vmem, vmem],
        out_specs=(pl.BlockSpec(memory_space=pl.ANY),) * 2 + (vmem,) * 3,
        scratch_shapes=[
            pltpu.VMEM((2 * core_rows, LANES), F32),
            pltpu.VMEM((half_q, depth), F32),
            pltpu.VMEM((half_p, depth), F32),
            pltpu.SemaphoreType.DMA((2, groups)),
        ],
        compiler_params=pltpu.CompilerParams(vmem_limit_bytes=VMEM_LAST),
        name="finish",
    )(limit, ours, theirs, logits)


def route(axes, move):
    sizes = [lax.axis_size(a) for a in axes]
    pairs = []
    for flat in range(math.prod(sizes)):
        left, where = flat, []
        for size in reversed(sizes):
            where.append(left % size)
            left //= size
        where = move(where[::-1], sizes)
        target = 0
        for place, size in zip(where, sizes):
            target = target * size + place
        pairs.append((flat, target))
    return pairs


GRID = ("hz", "hc", "wa")


def step(rows, cols):
    def move(where, sizes):
        high = (where[0] * sizes[1] + where[1] + rows) % (sizes[0] * sizes[1])
        return [high // sizes[1], high % sizes[1], (where[2] + cols) % sizes[2]]

    return move


FACE = ("hc", "wa", "ba")


def over(turn, by, crossed):
    def move(where, sizes):
        axis = 2 - (turn + (where[0] if crossed else 0)) % 2
        where = list(where)
        where[axis] = (where[axis] + by) % sizes[axis]
        return where

    return move


def along(by):
    return lambda where, sizes: [(where[0] + by) % sizes[0]]


def hand_out(blocks, place, axes, move):
    count = blocks.shape[0]
    total = lax.dynamic_index_in_dim(blocks, place, 0, keepdims=False).astype(F32)
    for by in range(count - 1, 0, -1):
        sent = lax.dynamic_index_in_dim(blocks, (place + by) % count, 0, keepdims=False)
        total = total + lax.ppermute(sent, axes, route(axes, move(by))).astype(F32)
    return total.astype(BF16)


def shards(tokens, cotangent, w_qkv, w_proj, table_logits, logit_scale, gain):
    images, rows, cols, depth = tokens.shape
    heads = logit_scale.shape[0]
    edge = WIN // 2
    both = jnp.concatenate([tokens, cotangent], 0)
    top = both[:, :edge]
    left = both[:, edge:, :edge].reshape(2, (rows - edge) * edge, depth)
    tip = both[:, :edge, :edge].reshape(2, edge * edge, depth)
    below = lax.ppermute(top, GRID, route(GRID, step(-1, 0)))
    right = lax.ppermute(left, GRID, route(GRID, step(0, -1)))
    corner = lax.ppermute(tip, GRID, route(GRID, step(-1, -1)))

    cores, tall, across = lax.axis_size("hc"), lax.axis_size("hz"), lax.axis_size("wa")
    images_over = lax.axis_size("ba")
    owners = cores * tall * across
    used = 2 * depth // LANES * depth + 2 * heads + depth // LANES + 1
    unit = 8 * owners
    sent = -(-used // unit) * unit
    crossed = images_over == across
    order = (images_over, across, crossed)
    call = make_kernel(rows, cols, depth, heads, sent, across, order)
    d_moved, mine, given = call(
        logit_scale, tokens, cotangent, below, right, corner, w_qkv, w_proj, table_logits, gain
    )

    right = lax.ppermute(d_moved[: rows - edge, cols - edge :], GRID, route(GRID, step(0, 1)))
    lower = lax.ppermute(d_moved[rows - edge :, : cols - edge], GRID, route(GRID, step(1, 0)))
    cross = lax.ppermute(
        d_moved[rows - edge :, cols - edge :], GRID, route(GRID, step(1, 1))
    )
    upper = jnp.concatenate([cross, lower], 1)
    main = jnp.concatenate([right, d_moved[: rows - edge, : cols - edge]], 1)
    back = jnp.concatenate([upper, main], 0)[None]
    d_tokens = (cotangent.astype(F32) + back.astype(F32)).astype(BF16)

    swap = route(("hc",), lambda where, sizes: [1 - where[0]])
    one = jnp.where(lax.axis_index("hc") < 0, 0.0, 1.0).astype(BF16)
    taken = lax.ppermute(given * one, "hc", swap)
    summed = (mine.astype(F32) + taken.astype(F32)).astype(BF16)
    piece = sent // owners
    core, column, image = lax.axis_index("hc"), lax.axis_index("wa"), lax.axis_index("ba")
    turn = core if crossed else 0
    moves = (lambda by: over(0, by, crossed)), (lambda by: over(1, by, crossed))
    summed = hand_out(summed, image + (column - image) * turn, FACE, moves[0])
    summed = hand_out(summed, column + (image - column) * turn, FACE, moves[1])
    summed = summed.reshape(tall, piece, LANES)
    total = hand_out(summed, lax.axis_index("hz"), ("hz",), along)
    spread = jnp.broadcast_to(total[None], (tall * across, piece, LANES))
    ours = lax.all_to_all(spread, ("wa", "hz"), 0, 0, tiled=True)
    ours = ours.reshape(sent // cores, LANES)
    theirs = lax.ppermute(ours, "hc", swap)
    d_wq, d_wp, d_table, d_scale, d_gain = finish(
        ours, theirs, table_logits, logit_scale, depth, heads
    )
    return (d_tokens, d_wq.T, d_wp.T, d_table, d_scale, d_gain)


def solution(mesh):
    sizes = mesh.shape
    devices = mesh.devices.reshape(sizes["ha"] // 2, 2, sizes["wa"], sizes["ba"])
    inner = Mesh(devices, ("hz", "hc", "wa", "ba"))
    image = P("ba", ("hz", "hc"), "wa", None)
    return jax.shard_map(
        shards,
        mesh=inner,
        in_specs=(image, image, P(), P(), P(), P(), P()),
        out_specs=(image, P(None, "ba"), P(None, "ba"), P(), P(), P()),
        check_vma=False,
    )
```
